8 devices in a mesh: dp: 1 (over z), col: 2 (over y), row: 4 (over x, core).
Axes of the slice: x: 2, y: 2, z: 1, core: 2. Of those that a mesh axis runs over, the one named last changes fastest.
Arguments:
- hidden: bfloat16 [128, 2560], P('dp', 'row')
- cache_len: int32 [128], P('dp')
- k_cache: bfloat16 [2, 128, 32, 256, 80], P(None, 'dp', ('col', 'row'))
- v_cache: bfloat16 [2, 128, 32, 256, 80], P(None, 'dp', ('col', 'row'))
- ln1_g: bfloat16 [2, 2560], P(None, 'row')
- ln1_b: bfloat16 [2, 2560], P(None, 'row')
- w_q: bfloat16 [2, 2560, 2560], P(None, 'row', 'col')
- b_q: bfloat16 [2, 2560], P(None, 'col')
- w_k: bfloat16 [2, 2560, 2560], P(None, 'row', 'col')
- b_k: bfloat16 [2, 2560], P(None, 'col')
- w_v: bfloat16 [2, 2560, 2560], P(None, 'row', 'col')
- b_v: bfloat16 [2, 2560], P(None, 'col')
- w_o: bfloat16 [2, 2560, 2560], P(None, 'col', 'row')
- b_o: bfloat16 [2, 2560], P(None, 'row')
- ln2_g: bfloat16 [2, 2560], P(None, 'row')
- ln2_b: bfloat16 [2, 2560], P(None, 'row')
- w_fc1: bfloat16 [2, 2560, 10240], P(None, 'row', 'col')
- b_fc1: bfloat16 [2, 10240], P(None, 'col')
- w_fc2: bfloat16 [2, 10240, 2560], P(None, 'col', 'row')
- b_fc2: bfloat16 [2, 2560], P(None, 'row')
Outputs:
- output 1: bfloat16 [128, 2560], P('dp', 'row')
- output 2: bfloat16 [2, 128, 32, 80], P(None, 'dp', ('col', 'row'))
- output 3: bfloat16 [2, 128, 32, 80], P(None, 'dp', ('col', 'row'))
All inputs are finite; a program needn't handle non-finite values.
Results may differ from the reference program's by a relative error of at most 0.0184677.
Values are sent between devices in bfloat16 or wider.
A program may use at most 1 GiB of HBM per device.

```python
import jax
import jax.numpy as jnp
from jax import lax

BATCH = 128
D_MODEL = 2560
HEADS = 32
S_MAX = 256
LAYERS = 2
HEAD_DIM = D_MODEL // HEADS
FF_DIM = 4 * D_MODEL
EPS_LN = 1e-5


def setup_inputs(seed: int = 0, part: int = 0) -> dict:
    shared_key = jax.random.key(seed)
    part_key = jax.random.fold_in(shared_key, part)
    part_keys = jax.random.split(part_key, 6)
    weight_keys = jax.random.split(shared_key, 16)

    def normal(rng_key, shape):
        return jax.random.normal(rng_key, shape, jnp.float32)

    def weight(rng_key, shape, fan_in, gain):
        return (gain * fan_in ** -0.5 * normal(rng_key, shape)).astype(jnp.bfloat16)

    def vector(rng_key, shape, center, spread):
        return (center + spread * normal(rng_key, shape)).astype(jnp.bfloat16)

    hidden = normal(part_keys[0], (BATCH, D_MODEL)) + 0.7 * normal(part_keys[1], (BATCH, 1))
    lengths = jax.random.randint(part_keys[2], (BATCH,), 0, S_MAX)
    lengths = lengths.at[0].set(S_MAX - 1).at[1].set(0)
    cache_shape = (LAYERS, BATCH, HEADS, S_MAX, HEAD_DIM)
    k_cache = 1.5 * normal(part_keys[3], cache_shape)
    v_cache = normal(part_keys[4], cache_shape) + 0.8 * normal(part_keys[5], (LAYERS, BATCH, HEADS, 1, HEAD_DIM))
    vec_shape = (LAYERS, D_MODEL)
    square_shape = (LAYERS, D_MODEL, D_MODEL)
    return {
        "hidden": hidden.astype(jnp.bfloat16),
        "cache_len": lengths.astype(jnp.int32),
        "k_cache": k_cache.astype(jnp.bfloat16),
        "v_cache": v_cache.astype(jnp.bfloat16),
        "ln1_g": vector(weight_keys[0], vec_shape, 1.0, 0.3),
        "ln1_b": vector(weight_keys[1], vec_shape, 0.0, 0.3),
        "w_q": weight(weight_keys[2], square_shape, D_MODEL, 1.5),
        "b_q": vector(weight_keys[3], vec_shape, 0.0, 0.5),
        "w_k": weight(weight_keys[4], square_shape, D_MODEL, 1.0),
        "b_k": vector(weight_keys[5], vec_shape, 0.0, 0.5),
        "w_v": weight(weight_keys[6], square_shape, D_MODEL, 1.0),
        "b_v": vector(weight_keys[7], vec_shape, 0.0, 0.5),
        "w_o": weight(weight_keys[8], square_shape, D_MODEL, 1.0),
        "b_o": vector(weight_keys[9], vec_shape, 0.0, 0.3),
        "ln2_g": vector(weight_keys[10], vec_shape, 1.0, 0.3),
        "ln2_b": vector(weight_keys[11], vec_shape, 0.0, 0.3),
        "w_fc1": weight(weight_keys[12], (LAYERS, D_MODEL, FF_DIM), D_MODEL, 1.0),
        "b_fc1": vector(weight_keys[13], (LAYERS, FF_DIM), 0.0, 0.5),
        "w_fc2": weight(weight_keys[14], (LAYERS, FF_DIM, D_MODEL), FF_DIM, 1.0),
        "b_fc2": vector(weight_keys[15], vec_shape, 0.0, 0.3),
    }


def layer_norm(state, gain, shift):
    state_f32 = state.astype(jnp.float32)
    mean_val = jnp.sum(state_f32, axis=-1, keepdims=True) / D_MODEL
    mean_sq = jnp.sum(state_f32 * state_f32, axis=-1, keepdims=True) / D_MODEL
    variance = mean_sq - mean_val * mean_val
    normed = (state_f32 - mean_val) * lax.rsqrt(variance + EPS_LN) * gain.astype(jnp.float32) + shift.astype(jnp.float32)
    return normed.astype(jnp.bfloat16)


def project(normed, weight, bias):
    return jnp.dot(normed, weight, preferred_element_type=jnp.float32) + bias.astype(jnp.float32)


def attend_row(row_args):
    q_row, k_row, v_row, k_fresh, v_fresh, length = row_args
    positions = jnp.arange(S_MAX)
    at_new = (positions == length)[None, :, None]
    keys_all = jnp.where(at_new, k_fresh[:, None, :], k_row)
    values_all = jnp.where(at_new, v_fresh[:, None, :], v_row)
    scores = jnp.einsum("hd,hsd->hs", q_row.astype(jnp.float32), keys_all.astype(jnp.float32))
    scores = jnp.where((positions <= length)[None, :], scores, -jnp.inf)
    probs = jax.nn.softmax(scores, axis=-1).astype(jnp.bfloat16)
    mixed = jnp.einsum("hs,hsd->hd", probs.astype(jnp.float32), values_all.astype(jnp.float32))
    return mixed.astype(jnp.bfloat16)


def reference(hidden, cache_len, k_cache, v_cache, ln1_g, ln1_b, w_q, b_q, w_k, b_k, w_v, b_v, w_o, b_o, ln2_g, ln2_b, w_fc1, b_fc1, w_fc2, b_fc2):
    scale = HEAD_DIM ** -0.5

    def layer_step(state, layer_args):
        (k_layer, v_layer, gain_one, shift_one, wq_layer, bq_layer, wk_layer, bk_layer, wv_layer, bv_layer,
         wo_layer, bo_layer, gain_two, shift_two, fc1_layer, bfc1_layer, fc2_layer, bfc2_layer) = layer_args
        normed = layer_norm(state, gain_one, shift_one)
        q_all = (project(normed, wq_layer, bq_layer) * scale).astype(jnp.bfloat16).reshape(BATCH, HEADS, HEAD_DIM)
        k_all = project(normed, wk_layer, bk_layer).astype(jnp.bfloat16).reshape(BATCH, HEADS, HEAD_DIM)
        v_all = project(normed, wv_layer, bv_layer).astype(jnp.bfloat16).reshape(BATCH, HEADS, HEAD_DIM)
        attended = lax.map(attend_row, (q_all, k_layer, v_layer, k_all, v_all, cache_len))
        state_mid = (state.astype(jnp.float32) + project(attended.reshape(BATCH, D_MODEL), wo_layer, bo_layer)).astype(jnp.bfloat16)
        normed_two = layer_norm(state_mid, gain_two, shift_two)
        inner = jnp.maximum(project(normed_two, fc1_layer, bfc1_layer).astype(jnp.bfloat16), 0)
        state_out = (state_mid.astype(jnp.float32) + project(inner, fc2_layer, bfc2_layer)).astype(jnp.bfloat16)
        return state_out, (k_all, v_all)

    layer_inputs = (k_cache, v_cache, ln1_g, ln1_b, w_q, b_q, w_k, b_k, w_v, b_v, w_o, b_o, ln2_g, ln2_b, w_fc1, b_fc1, w_fc2, b_fc2)
    state_final, fresh_rows = lax.scan(layer_step, hidden, layer_inputs)
    return state_final, fresh_rows[0], fresh_rows[1]
```

```python
import functools

import jax
import jax.numpy as jnp
from jax import lax
from jax.experimental import pallas as pl
from jax.experimental.pallas import tpu as pltpu
from jax.sharding import PartitionSpec as P

EPS_LN = 1e-5
F32 = jnp.float32
BF16 = jnp.bfloat16
STREAMS = 2
RING = 12
CB = 8
CW = 512
MESH = pl.DeviceIdType.MESH


def fused(dims, hid_ref, len_ref, k_hbm, v_hbm, g1_ref, c1_ref, wq_hbm, bq_ref, wk_hbm, bk_ref, wv_hbm, bv_ref,
          wo_hbm, bo_ref, g2_ref, c2_ref, f1_hbm, bf1_ref, f2_hbm, bf2_ref,
          out_ref, kt_ref, vt_ref,
          kbuf, vbuf, wqkv, wo, wf1, wf2,
          state, ynorm, st_send, st_recv,
          qd_send, qd_recv, q_mine, qx_send, qx_recv,
          qblk, vexp, snew, o_rows, att, kfull, vfull,
          ysend, yrecv, acc,
          fd_send, fd_recv, f_mine, fx_send, fx_recv, u_buf,
          kv_sem, w_sem, st_ssem, st_rsem, qd_ssem, qd_rsem, qx_ssem, qx_rsem,
          at_ssem, at_rsem, y_ssem, y_rsem, fd_ssem, fd_rsem, fx_ssem, fx_rsem, u_ssem, u_rsem):
    layers, batch, dm, hw, heads, s_max = dims
    hd = hw // heads
    d_total = dm * 4
    rows = batch // STREAMS
    nchunk = rows // CB
    total_chunks = layers * STREAMS * nchunk
    ff_half = wf1.shape[1] // 2
    nj = ff_half // CW

    r = lax.axis_index("row")
    c = lax.axis_index("col")
    core = lax.rem(r, 2)
    chip = r // 2
    partner = r + 1 - 2 * core
    xpeer = lax.rem(r + 2, 4)
    diag = lax.rem(partner + 2, 4)
    dev_p = {"row": partner}
    dev_x = {"row": xpeer}
    dev_d = {"row": diag}
    dev_y = {"col": 1 - c}

    def rcopy(src, dst, ssem, rsem, dev):
        return pltpu.make_async_remote_copy(src_ref=src, dst_ref=dst, send_sem=ssem, recv_sem=rsem,
                                            device_id=dev, device_id_type=MESH)

    def kv_copies(ci):
        layer = ci // (STREAMS * nchunk)
        first = lax.rem(ci, STREAMS * nchunk) * CB
        slot = lax.rem(ci, RING)
        return (pltpu.make_async_copy(k_hbm.at[layer, pl.ds(first, CB)], kbuf.at[slot], kv_sem.at[0, slot]),
                pltpu.make_async_copy(v_hbm.at[layer, pl.ds(first, CB)], vbuf.at[slot], kv_sem.at[1, slot]))

    def w_copies(name, layer):
        if name == "qkv":
            return [pltpu.make_async_copy(w.at[layer], wqkv.at[i], w_sem.at[i])
                    for i, w in enumerate((wq_hbm, wk_hbm, wv_hbm))]
        src, dst, i = {"o": (wo_hbm, wo, 3), "f1": (f1_hbm, wf1, 4), "f2": (f2_hbm, wf2, 5)}[name]
        return [pltpu.make_async_copy(src.at[layer], dst, w_sem.at[i])]

    def w_start(name, layer):
        if layer < layers:
            for cp in w_copies(name, layer):
                cp.start()

    def w_wait(name, layer):
        for cp in w_copies(name, layer):
            cp.wait()

    w_start("qkv", 0)

    def prime(ci, carry):
        for cp in kv_copies(ci):
            cp.start()
        return carry

    lax.fori_loop(0, RING, prime, 0)

    barrier = pltpu.get_barrier_semaphore()
    for dev in (dev_p, dev_x, dev_d, dev_y):
        pl.semaphore_signal(barrier, inc=1, device_id=dev, device_id_type=MESH)
    pl.semaphore_wait(barrier, 4)

    def rsl(s):
        return pl.ds(s * rows, rows)

    def stat_copies(s, which):
        return [rcopy(st_send.at[which, s], st_recv.at[which, s, i], st_ssem.at[which, s, i], st_rsem.at[which, s, i], dev)
                for i, dev in enumerate((dev_p, dev_x, dev_d))]

    def stats_send(s, which, xv):
        p1 = xv[:, 0:128]
        p2 = p1 * p1
        for i in range(1, dm // 128):
            t = xv[:, i * 128:(i + 1) * 128]
            p1 = p1 + t
            p2 = p2 + t * t
        both = jnp.concatenate([p1, p2], axis=0)
        row = jnp.sum(both.T, axis=0, keepdims=True)
        st_send[which, s] = jnp.broadcast_to(row, (8, 2 * rows))
        for cp in stat_copies(s, which):
            cp.start()

    def norm(s, which, gain, shift):
        for cp in stat_copies(s, which):
            cp.wait()
        row = ((st_send[which, s, 0:1, :] + st_recv[which, s, 0, 0:1, :])
               + (st_recv[which, s, 1, 0:1, :] + st_recv[which, s, 2, 0:1, :]))
        n2 = 2 * rows
        eye = lax.broadcasted_iota(jnp.int32, (n2, n2), 0) == lax.broadcasted_iota(jnp.int32, (n2, n2), 1)
        col = jnp.sum(jnp.where(eye, jnp.broadcast_to(row, (n2, n2)), 0.0), axis=1, keepdims=True)
        mean = col[0:rows] * (1.0 / d_total)
        var = col[rows:] * (1.0 / d_total) - mean * mean
        rstd = lax.rsqrt(var + EPS_LN)
        xv = state[rsl(s), :].astype(F32)
        ynorm[rsl(s), :] = ((xv - mean) * rstd * gain.astype(F32) + shift.astype(F32)).astype(BF16)

    def qd_copy(s, i):
        return rcopy(qd_send.at[s, i], qd_recv.at[s, i], qd_ssem.at[s, i], qd_rsem.at[s, i], dev_p)

    def qx_copy(s):
        return rcopy(qx_send.at[s], qx_recv.at[s], qx_ssem.at[s], qx_rsem.at[s], dev_x)

    def qkv_part(s, layer):
        yv = ynorm[rsl(s), :]
        for i, target in enumerate((1 - chip, chip)):
            off = pl.multiple_of(target * (2 * hw), 128)
            for m in range(3):
                res = jnp.dot(yv, wqkv[m, :, pl.ds(off, 2 * hw)], preferred_element_type=F32)
                low, high = res[:, :hw], res[:, hw:]
                q_mine[s, i, :, m * hw:(m + 1) * hw] = jnp.where(core == 0, low, high)
                qd_send[s, i, :, m * hw:(m + 1) * hw] = jnp.where(core == 0, high, low).astype(BF16)
            qd_copy(s, i).start()

    def qkv_forward(s):
        qd_copy(s, 0).wait()
        qx_send[s] = (q_mine[s, 0] + qd_recv[s, 0].astype(F32)).astype(BF16)
        qx_copy(s).start()

    def own_bias(b_ref, layer):
        b = b_ref[layer:layer + 1, :].astype(F32)
        parts = [b[:, i * hw:(i + 1) * hw] for i in range(4)]
        return jnp.where(r == 0, parts[0], jnp.where(r == 1, parts[1], jnp.where(r == 2, parts[2], parts[3])))

    def expand_mat(dtype):
        hr = heads * rows
        return (lax.broadcasted_iota(jnp.int32, (hr, rows), 0) // heads
                == lax.broadcasted_iota(jnp.int32, (hr, rows), 1)).astype(F32).astype(dtype)

    def head_mask(n):
        row = lax.rem(lax.broadcasted_iota(jnp.int32, (n, hw), 0), heads)
        lane = lax.broadcasted_iota(jnp.int32, (n, hw), 1)
        return (lane >= row * hd) & (lane < row * hd + hd)

    def qkv_finish(s, layer):
        qd_copy(s, 1).wait()
        qx_copy(s).wait()
        tot = (q_mine[s, 1] + qd_recv[s, 1].astype(F32)) + qx_recv[s].astype(F32)
        q = ((tot[:, 0:hw] + own_bias(bq_ref, layer)) * (hd ** -0.5)).astype(BF16)
        k = (tot[:, hw:2 * hw] + own_bias(bk_ref, layer)).astype(BF16)
        v = (tot[:, 2 * hw:3 * hw] + own_bias(bv_ref, layer)).astype(BF16)
        kfull[rsl(s), :hw] = k.astype(F32)
        vfull[rsl(s), :hw] = v.astype(F32)
        ex = expand_mat(BF16)
        hm = head_mask(heads * rows)
        qe = jnp.where(hm, jnp.dot(ex, q, preferred_element_type=F32), 0.0)
        ke = jnp.dot(ex, k, preferred_element_type=F32)
        vexp[...] = jnp.dot(ex, v, preferred_element_type=F32)
        qblk[...] = qe.astype(BF16)
        snew[...] = jnp.broadcast_to(jnp.sum(qe * ke, axis=1, keepdims=True), snew.shape)

    def attention(s, layer):
        base = (layer * STREAMS + s) * nchunk
        r8 = lax.broadcasted_iota(jnp.int32, (8, 1), 0)
        upper = r8 < heads
        nr = CB * heads
        pos = lax.broadcasted_iota(jnp.int32, (nr, s_max), 1)
        hm = head_mask(nr)

        def body(g, carry):
            ci = base + g
            slot = lax.rem(ci, RING)
            for cp in kv_copies(ci):
                cp.wait()
            row0 = pl.multiple_of(g * nr, nr)
            sc = []
            lens = []
            for t in range(nr // 16):
                lhs = qblk[pl.ds(pl.multiple_of(row0 + t * 16, 16), 16), :]
                d = [jnp.dot(lhs, kbuf[slot, t * 4 + i], preferred_element_type=F32) for i in range(4)]
                sc.append(jnp.where(upper, d[0][0:8], d[1][0:8]))
                sc.append(jnp.where(upper, d[2][8:16], d[3][8:16]))
                ln = [len_ref[s * rows + g * CB + t * 4 + i] for i in range(4)]
                lens.append(jnp.where(upper, ln[0], ln[1]))
                lens.append(jnp.where(upper, ln[2], ln[3]))
            scores = jnp.concatenate(sc, axis=0)
            length = jnp.concatenate(lens, axis=0)
            scores = jnp.where(pos < length, scores, -jnp.inf)
            sn = snew[pl.ds(row0, nr), 0:1]
            peak = jnp.maximum(jnp.max(scores, axis=1, keepdims=True), sn)
            e = jnp.exp(scores - peak)
            en = jnp.exp(sn - peak)
            inv = 1.0 / (jnp.sum(e, axis=1, keepdims=True) + en)
            prob = (e * inv).astype(BF16)
            pn = (en * inv).astype(BF16).astype(F32)
            o = []
            for t in range(nr // 16):
                lhs = prob[t * 16:(t + 1) * 16]
                d = [lax.dot_general(lhs, vbuf[slot, t * 4 + i], (((1,), (1,)), ((), ())), preferred_element_type=F32)
                     for i in range(4)]
                o.append(jnp.where(upper, d[0][0:8], d[1][0:8]))
                o.append(jnp.where(upper, d[2][8:16], d[3][8:16]))
            mixed = jnp.concatenate(o, axis=0) + pn * vexp[pl.ds(row0, nr), :]
            o_rows[pl.ds(row0, nr), :] = jnp.where(hm, mixed, 0.0).astype(BF16)

            @pl.when(ci + RING < total_chunks)
            def _():
                for cp in kv_copies(ci + RING):
                    cp.start()
            return carry

        lax.fori_loop(0, nchunk, body, 0)

    def att_copies(s):
        mine = att.at[s, 0]
        return (rcopy(mine, att.at[s, 1], at_ssem.at[s, 0], at_rsem.at[s, 0], dev_p),
                rcopy(mine, att.at[s, 2], at_ssem.at[s, 1], at_rsem.at[s, 1], dev_x),
                rcopy(att.at[s, 2], att.at[s, 3], at_ssem.at[s, 2], at_rsem.at[s, 2], dev_p))

    def att_send(s):
        hr = heads * rows
        sel = (lax.broadcasted_iota(jnp.int32, (rows, hr), 1) // heads
               == lax.broadcasted_iota(jnp.int32, (rows, hr), 0)).astype(F32).astype(BF16)
        att[s, 0] = jnp.dot(sel, o_rows[...], preferred_element_type=F32).astype(BF16)
        a, b, _ = att_copies(s)
        b.start()
        a.start()

    def att_relay(s):
        _, b, f = att_copies(s)
        b.wait_recv()
        f.start()

    def y_copy(s, which):
        return rcopy(ysend.at[which, s], yrecv.at[which, s], y_ssem.at[which, s], y_rsem.at[which, s], dev_y)

    def out_proj(s):
        a, b, f = att_copies(s)
        a.wait()
        b.wait_send()
        f.wait()
        res = None
        for i, owner in enumerate((r, partner, xpeer, diag)):
            off = pl.multiple_of(owner * hw, 16)
            t = jnp.dot(att[s, i], wo[pl.ds(off, hw), :], preferred_element_type=F32)
            res = t if res is None else res + t
        ysend[0, s] = res.astype(BF16)
        y_copy(s, 0).start()

    def residual(s, which, bias):
        y_copy(s, which).wait()
        both = ysend[which, s].astype(F32) + yrecv[which, s].astype(F32)
        new = (state[rsl(s), :].astype(F32) + (both + bias.astype(F32))).astype(BF16)
        return new

    def fd_copy(s, j):
        return rcopy(fd_send.at[s, j], fd_recv.at[s, j], fd_ssem.at[s, j], fd_rsem.at[s, j], dev_p)

    def fx_copy(s, j):
        return rcopy(fx_send.at[s, j], fx_recv.at[s, j], fx_ssem.at[s, j], fx_rsem.at[s, j], dev_x)

    def u_copy(s, j, owner):
        return rcopy(u_buf.at[s, owner, j], u_buf.at[s, owner, j], u_ssem.at[s, j], u_rsem.at[s, j], dev_p)

    def fc1_part(s):
        yv = ynorm[rsl(s), :]

        def body(j, carry):
            off = pl.multiple_of((1 - core) * ff_half + j * CW, 128)
            fd_send[s, j] = jnp.dot(yv, wf1[:, pl.ds(off, CW)], preferred_element_type=F32).astype(BF16)
            fd_copy(s, j).start()
            off = pl.multiple_of(core * ff_half + j * CW, 128)
            f_mine[s, j] = jnp.dot(yv, wf1[:, pl.ds(off, CW)], preferred_element_type=F32)
            return carry

        lax.fori_loop(0, nj, body, 0)

    def fc1_forward(s):
        def body(j, carry):
            fd_copy(s, j).wait()
            fx_send[s, j] = (f_mine[s, j] + fd_recv[s, j].astype(F32)).astype(BF16)
            fx_copy(s, j).start()
            return carry

        lax.fori_loop(0, nj, body, 0)

    def fc2_add(s, j, owner):
        off = pl.multiple_of(owner * ff_half + j * CW, 128)
        acc[s] += jnp.dot(u_buf[s, owner, j], wf2[pl.ds(off, CW), :], preferred_element_type=F32)

    def mlp(s, layer, lo, hi):
        if lo == 0:
            acc[s] = jnp.zeros(acc.shape[1:], F32)

        def body(j, carry):
            fx_copy(s, j).wait()
            off = pl.multiple_of(core * ff_half + j * CW, 128)
            bias = bf1_ref[layer:layer + 1, pl.ds(off, CW)].astype(F32)
            u = ((fx_send[s, j].astype(F32) + fx_recv[s, j].astype(F32)) + bias).astype(BF16)
            u_buf[s, core, j] = jnp.maximum(u, jnp.zeros_like(u))
            u_copy(s, j, core).start()
            fc2_add(s, j, core)

            @pl.when(j > 0)
            def _():
                u_copy(s, j - 1, 1 - core).wait_recv()
                fc2_add(s, j - 1, 1 - core)
            return carry

        lax.fori_loop(lo, hi, body, 0)
        if hi == nj:
            u_copy(s, nj - 1, 1 - core).wait_recv()
            fc2_add(s, nj - 1, 1 - core)

            def drain(j, carry):
                u_copy(s, j, core).wait_send()
                return carry

            lax.fori_loop(0, nj, drain, 0)
            ysend[1, s] = acc[s].astype(BF16)
            y_copy(s, 1).start()

    def kv_out(layer):
        kt_ref[layer] = kfull[...].T[:hw, :].astype(BF16)
        vt_ref[layer] = vfull[...].T[:hw, :].astype(BF16)

    kfull[...] = jnp.zeros_like(kfull)
    vfull[...] = jnp.zeros_like(vfull)
    state[...] = hid_ref[...]
    S = range(STREAMS)
    for s in S:
        stats_send(s, 0, state[rsl(s), :].astype(F32))
    for layer in range(layers):
        last = layer == layers - 1
        w_wait("qkv", layer)
        for s in S:
            norm(s, 0, g1_ref[layer:layer + 1, :], c1_ref[layer:layer + 1, :])
            qkv_part(s, layer)
        w_start("qkv", layer + 1)
        if layer == 0:
            w_start("o", 0)
            w_start("f1", 0)
            w_start("f2", 0)
        for s in S:
            qkv_forward(s)
        for s in S:
            qkv_finish(s, layer)
            attention(s, layer)
            att_send(s)
        kv_out(layer)
        for s in S:
            att_relay(s)
        w_wait("o", layer)
        for s in S:
            out_proj(s)
        w_start("o", layer + 1)
        for s in S:
            new = residual(s, 0, bo_ref[layer:layer + 1, :])
            state[rsl(s), :] = new
            stats_send(s, 1, new.astype(F32))
        w_wait("f1", layer)
        for s in S:
            norm(s, 1, g2_ref[layer:layer + 1, :], c2_ref[layer:layer + 1, :])
            fc1_part(s)
            fc1_forward(s)
        w_start("f1", layer + 1)
        w_wait("f2", layer)
        for s in S:
            mlp(s, layer, 0, nj)
        w_start("f2", layer + 1)
        for s in S:
            new = residual(s, 1, bf2_ref[layer:layer + 1, :])
            if last:
                out_ref[rsl(s), :] = new
            else:
                state[rsl(s), :] = new
                stats_send(s, 0, new.astype(F32))


def solution(mesh):
    act_spec = P("dp", "row")
    cache_spec = P(None, "dp", ("col", "row"), None, None)
    fresh_spec = P(None, "dp", ("col", "row"), None)
    in_weight = P(None, "row", "col")
    out_weight = P(None, "col", "row")
    col_vec = P(None, "col")
    row_vec = P(None, "row")
    in_specs = (act_spec, P("dp"), cache_spec, cache_spec, row_vec, row_vec,
                in_weight, col_vec, in_weight, col_vec, in_weight, col_vec,
                out_weight, row_vec, row_vec, row_vec, in_weight, col_vec, out_weight, row_vec)

    def local_step(hidden, cache_len, k_cache, v_cache, ln1_g, ln1_b, w_q, b_q, w_k, b_k, w_v, b_v,
                   w_o, b_o, ln2_g, ln2_b, w_fc1, b_fc1, w_fc2, b_fc2):
        layers, batch, heads, s_max, hd = k_cache.shape
        dm = hidden.shape[1]
        hw = heads * hd
        ff = w_fc1.shape[2]
        rows = batch // STREAMS
        nj = ff // 2 // CW
        kt = k_cache.transpose(0, 1, 2, 4, 3).reshape(layers, batch, hw, s_max)
        vt = v_cache.transpose(0, 1, 2, 4, 3).reshape(layers, batch, hw, s_max)
        vm = pl.BlockSpec(memory_space=pltpu.VMEM)
        hb = pl.BlockSpec(memory_space=pl.ANY)
        sm = pl.BlockSpec(memory_space=pltpu.SMEM)
        hr = heads * rows
        V = pltpu.VMEM
        D = pltpu.SemaphoreType.DMA
        scratch = [
            V((RING, CB, hw, s_max), BF16), V((RING, CB, hw, s_max), BF16),
            V((3,) + w_q.shape[1:], BF16), V(w_o.shape[1:], BF16), V(w_fc1.shape[1:], BF16), V(w_fc2.shape[1:], BF16),
            V((batch, dm), BF16), V((batch, dm), BF16),
            V((2, STREAMS, 8, 2 * rows), F32), V((2, STREAMS, 3, 8, 2 * rows), F32),
            V((STREAMS, 2, rows, 3 * hw), BF16), V((STREAMS, 2, rows, 3 * hw), BF16), V((STREAMS, 2, rows, 3 * hw), F32),
            V((STREAMS, rows, 3 * hw), BF16), V((STREAMS, rows, 3 * hw), BF16),
            V((hr, hw), BF16), V((hr, hw), F32), V((hr, 128), F32), V((hr, hw), BF16),
            V((STREAMS, 4, rows, hw), BF16), V((batch, 384), F32), V((batch, 384), F32),
            V((2, STREAMS, rows, dm), BF16), V((2, STREAMS, rows, dm), BF16), V((STREAMS, rows, dm), F32),
            V((STREAMS, nj, rows, CW), BF16), V((STREAMS, nj, rows, CW), BF16), V((STREAMS, nj, rows, CW), F32),
            V((STREAMS, nj, rows, CW), BF16), V((STREAMS, nj, rows, CW), BF16), V((STREAMS, 2, nj, rows, CW), BF16),
            D((2, RING)), D((6,)), D((2, STREAMS, 3)), D((2, STREAMS, 3)),
            D((STREAMS, 2)), D((STREAMS, 2)), D((STREAMS,)), D((STREAMS,)),
            D((STREAMS, 3)), D((STREAMS, 3)), D((2, STREAMS)), D((2, STREAMS)),
            D((STREAMS, nj)), D((STREAMS, nj)), D((STREAMS, nj)), D((STREAMS, nj)), D((STREAMS, nj)), D((STREAMS, nj)),
        ]
        out, kn, vn = pl.pallas_call(
            functools.partial(fused, (layers, batch, dm, hw, heads, s_max)),
            out_shape=(jax.ShapeDtypeStruct((batch, dm), BF16),
                       jax.ShapeDtypeStruct((layers, hw, batch), BF16),
                       jax.ShapeDtypeStruct((layers, hw, batch), BF16)),
            in_specs=[vm, sm, hb, hb, vm, vm, hb, vm, hb, vm, hb, vm, hb, vm, vm, vm, hb, vm, hb, vm],
            out_specs=(vm, vm, vm),
            scratch_shapes=scratch,
            compiler_params=pltpu.CompilerParams(collective_id=0, has_side_effects=True,
                                                 vmem_limit_bytes=67043328),
        )(hidden, cache_len, kt, vt, ln1_g, ln1_b, w_q, b_q, w_k, b_k, w_v, b_v,
          w_o, b_o, ln2_g, ln2_b, w_fc1, b_fc1, w_fc2, b_fc2)
        kn = kn.reshape(layers, heads, hd, batch).transpose(0, 3, 1, 2)
        vn = vn.reshape(layers, heads, hd, batch).transpose(0, 3, 1, 2)
        return out, kn, vn

    return jax.shard_map(local_step, mesh=mesh, in_specs=in_specs,
                         out_specs=(act_spec, fresh_spec, fresh_spec), check_vma=False)
```

```python
import functools

import jax
import jax.numpy as jnp
from jax import lax
from jax.experimental import pallas as pl
from jax.experimental.pallas import tpu as pltpu
from jax.sharding import PartitionSpec as P

EPS_LN = 1e-5
F32 = jnp.float32
BF16 = jnp.bfloat16
STREAMS = 2
RING = 12
CB = 8
CW = 512
MESH = pl.DeviceIdType.MESH
LANES = 128


def wide(tiles):
    return jnp.concatenate(tiles, axis=1)


def fused(dims, hid_ref, len_ref, k_hbm, v_hbm, g1_ref, c1_ref, wq_hbm, bq_ref, wk_hbm, bk_ref, wv_hbm, bv_ref,
          wo_hbm, bo_ref, g2_ref, c2_ref, f1_hbm, bf1_ref, f2_hbm, bf2_ref,
          out_ref, kt_ref, vt_ref,
          kbuf, vbuf, wqkv, wo, wf1, wf2,
          state, ynorm, st_send, st_recv,
          qd_send, qd_recv, q_mine, qx_send, qx_recv,
          qblk, snew, sbuf, pbuf, pnew, tmix, att, kfull, vfull,
          ysend, yrecv, acc,
          fd_send, fd_recv, f_mine, fx_send, fx_recv, u_buf,
          kv_sem, wq_sem, wo_sem, f1_sem, f2_sem, st_ssem, st_rsem, qd_ssem, qd_rsem, qx_ssem, qx_rsem,
          at_ssem, at_rsem, y_ssem, y_rsem, fd_ssem, fd_rsem, fx_ssem, fx_rsem, u_ssem, u_rsem):
    layers, batch, dm, hw, heads, s_max, ff = dims
    hd = hw // heads
    d_total = dm * 4
    rows = batch // STREAMS
    nchunk = rows // CB
    total_chunks = layers * STREAMS * nchunk
    ff_half = ff // 2
    nt = dm // LANES
    ct = CW // LANES
    nj = ff_half // CW

    r = lax.axis_index("row")
    c = lax.axis_index("col")
    core = lax.rem(r, 2)
    chip = r // 2
    partner = r + 1 - 2 * core
    xpeer = lax.rem(r + 2, 4)
    diag = lax.rem(partner + 2, 4)
    dev_p = {"row": partner}
    dev_x = {"row": xpeer}
    dev_d = {"row": diag}
    dev_y = {"col": 1 - c}

    def rcopy(src, dst, ssem, rsem, dev):
        return pltpu.make_async_remote_copy(src_ref=src, dst_ref=dst, send_sem=ssem, recv_sem=rsem,
                                            device_id=dev, device_id_type=MESH)

    def kv_copies(ci, i):
        layer = ci // (STREAMS * nchunk)
        first = lax.rem(ci, STREAMS * nchunk) * CB
        slot = lax.rem(ci, RING)
        src, dst = ((k_hbm, kbuf), (v_hbm, vbuf))[i]
        return [pltpu.make_async_copy(src.at[layer, pl.ds(first, CB), :, pl.ds(h * LANES, LANES)], dst.at[slot, :, h],
                                      kv_sem.at[i, h, slot]) for h in range(s_max // LANES)]

    def kv_start(ci, i):
        for cp in kv_copies(ci, i):
            cp.start()

    def kv_wait(ci, i):
        for cp in kv_copies(ci, i):
            cp.wait()

    def w_each(name, layer, act):
        def run(src, dst, sems, tiles):
            def body(t, carry):
                cp = pltpu.make_async_copy(src.at[layer, :, pl.ds(pl.multiple_of(t * LANES, LANES), LANES)], dst(t), sems(t))
                cp.start() if act else cp.wait()
                return carry
            lax.fori_loop(0, tiles, body, 0)

        if name == "qkv":
            for i, w in enumerate((wq_hbm, wk_hbm, wv_hbm)):
                run(w, lambda t, i=i: wqkv.at[t // nt, i * nt + lax.rem(t, nt)], lambda t, i=i: wq_sem.at[i, t], 2 * nt)
        elif name == "o":
            run(wo_hbm, lambda t: wo.at[t], lambda t: wo_sem.at[t], nt)
        elif name == "f1":
            run(f1_hbm, lambda t: wf1.at[t], lambda t: f1_sem.at[t], ff // LANES)
        else:
            run(f2_hbm, lambda t: wf2.at[t], lambda t: f2_sem.at[t], nt)

    def w_start(name, layer):
        if layer < layers:
            w_each(name, layer, True)

    def w_wait(name, layer):
        w_each(name, layer, False)

    w_start("qkv", 0)

    def prime(ci, carry):
        kv_start(ci, 0)
        kv_start(ci, 1)
        return carry

    lax.fori_loop(0, RING, prime, 0)

    barrier = pltpu.get_barrier_semaphore()
    for dev in (dev_p, dev_x, dev_d, dev_y):
        pl.semaphore_signal(barrier, inc=1, device_id=dev, device_id_type=MESH)
    pl.semaphore_wait(barrier, 4)

    def rsl(s):
        return pl.ds(s * rows, rows)

    def stat_copies(s, which):
        return [rcopy(st_send.at[which, s], st_recv.at[which, s, i], st_ssem.at[which, s, i], st_rsem.at[which, s, i], dev)
                for i, dev in enumerate((dev_p, dev_x, dev_d))]

    def stats_send(s, which, xv):
        p1 = xv[:, 0:128]
        p2 = p1 * p1
        for i in range(1, dm // 128):
            t = xv[:, i * 128:(i + 1) * 128]
            p1 = p1 + t
            p2 = p2 + t * t
        both = jnp.concatenate([p1, p2], axis=0)
        row = jnp.sum(both.T, axis=0, keepdims=True)
        st_send[which, s] = jnp.broadcast_to(row, (8, 2 * rows))
        for cp in stat_copies(s, which):
            cp.start()

    def norm(s, which, gain, shift):
        for cp in stat_copies(s, which):
            cp.wait()
        row = ((st_send[which, s, 0:1, :] + st_recv[which, s, 0, 0:1, :])
               + (st_recv[which, s, 1, 0:1, :] + st_recv[which, s, 2, 0:1, :]))
        n2 = 2 * rows
        eye = lax.broadcasted_iota(jnp.int32, (n2, n2), 0) == lax.broadcasted_iota(jnp.int32, (n2, n2), 1)
        col = jnp.sum(jnp.where(eye, jnp.broadcast_to(row, (n2, n2)), 0.0), axis=1, keepdims=True)
        mean = col[0:rows] * (1.0 / d_total)
        var = col[rows:] * (1.0 / d_total) - mean * mean
        rstd = lax.rsqrt(var + EPS_LN)
        xv = state[rsl(s), :].astype(F32)
        y = ((xv - mean) * rstd * gain.astype(F32) + shift.astype(F32)).astype(BF16)
        for t in range(nt):
            ynorm[t, rsl(s), :] = y[:, t * LANES:(t + 1) * LANES]

    def normed(s):
        return wide([ynorm[t, rsl(s), :] for t in range(nt)])

    def qd_copy(s, i):
        return rcopy(qd_send.at[s, i], qd_recv.at[s, i], qd_ssem.at[s, i], qd_rsem.at[s, i], dev_p)

    def qx_copy(s):
        return rcopy(qx_send.at[s], qx_recv.at[s], qx_ssem.at[s], qx_rsem.at[s], dev_x)

    def qkv_part(s, i):
        target = 1 - chip if i == 0 else chip
        res = jnp.dot(normed(s), wide([wqkv[target, t] for t in range(3 * nt)]), preferred_element_type=F32)
        for m in range(3):
            low, high = res[:, 2 * m * hw:(2 * m + 1) * hw], res[:, (2 * m + 1) * hw:(2 * m + 2) * hw]
            q_mine[s, i, :, m * hw:(m + 1) * hw] = jnp.where(core == 0, low, high)
            qd_send[s, i, :, m * hw:(m + 1) * hw] = jnp.where(core == 0, high, low).astype(BF16)
        qd_copy(s, i).start()

    def qkv_forward(s):
        qd_copy(s, 0).wait()
        qx_send[s] = (q_mine[s, 0] + qd_recv[s, 0].astype(F32)).astype(BF16)
        qx_copy(s).start()

    def own_bias(b_ref, layer):
        b = b_ref[layer:layer + 1, :].astype(F32)
        parts = [b[:, i * hw:(i + 1) * hw] for i in range(4)]
        return jnp.where(r == 0, parts[0], jnp.where(r == 1, parts[1], jnp.where(r == 2, parts[2], parts[3])))

    def expand_mat():
        hr = heads * rows
        return (lax.broadcasted_iota(jnp.int32, (hr, rows), 0) // heads
                == lax.broadcasted_iota(jnp.int32, (hr, rows), 1)).astype(F32).astype(BF16)

    def head_mask(n):
        row = lax.rem(lax.broadcasted_iota(jnp.int32, (n, hw), 0), heads)
        lane = lax.broadcasted_iota(jnp.int32, (n, hw), 1)
        return (lane >= row * hd) & (lane < row * hd + hd)

    def qkv_finish(s, layer):
        qd_copy(s, 1).wait()
        qx_copy(s).wait()
        tot = (q_mine[s, 1] + qd_recv[s, 1].astype(F32)) + qx_recv[s].astype(F32)
        q = ((tot[:, 0:hw] + own_bias(bq_ref, layer)) * (hd ** -0.5)).astype(BF16)
        k = (tot[:, hw:2 * hw] + own_bias(bk_ref, layer)).astype(BF16)
        v = (tot[:, 2 * hw:3 * hw] + own_bias(bv_ref, layer)).astype(BF16)
        kfull[rsl(s), :hw] = k.astype(F32)
        vfull[rsl(s), :hw] = v.astype(F32)
        ex = expand_mat()
        hm = head_mask(heads * rows)
        qe = jnp.where(hm, jnp.dot(ex, q, preferred_element_type=F32), 0.0)
        ke = jnp.dot(ex, k, preferred_element_type=F32)
        qblk[...] = qe.astype(BF16)
        snew[...] = jnp.broadcast_to(jnp.sum(qe * ke, axis=1, keepdims=True), snew.shape)

    nr = CB * heads
    per = 128 // nr
    upper = lax.broadcasted_iota(jnp.int32, (8, 1), 0) < heads

    pos = lax.broadcasted_iota(jnp.int32, (nr, s_max), 1)

    def at_row(g):
        return pl.multiple_of(g * nr, nr)

    def scores_of(base, g):
        slot = lax.rem(base + g, RING)
        out = []
        for t in range(nr // 16):
            lhs = qblk[pl.ds(pl.multiple_of(at_row(g) + t * 16, 16), 16), :]
            d = [jnp.dot(lhs, wide([kbuf[slot, t * 4 + i, h] for h in range(s_max // LANES)]), preferred_element_type=F32)
                 for i in range(4)]
            out.append(jnp.where(upper, d[0][0:8], d[1][0:8]))
            out.append(jnp.where(upper, d[2][8:16], d[3][8:16]))
        return jnp.concatenate(out, axis=0)

    def softmax_of(s, g, sc):
        lens = []
        for i in range(0, CB, 2):
            b = s * rows + g * CB + i
            lens.append(jnp.where(upper, len_ref[b], len_ref[b + 1]))
        sc = jnp.where(pos < jnp.concatenate(lens, axis=0), sc, -jnp.inf)
        sn = snew[pl.ds(at_row(g), nr), 0:1]
        peak = jnp.maximum(jnp.max(sc, axis=1, keepdims=True), sn)
        e = jnp.exp(sc - peak)
        en = jnp.exp(sn - peak)
        inv = 1.0 / (jnp.sum(e, axis=1, keepdims=True) + en)
        return (e * inv).astype(BF16), jnp.broadcast_to(en * inv, (nr, LANES))

    def keep_probs(g, prob, fresh):
        for h in range(s_max // LANES):
            pbuf[h, pl.ds(at_row(g), nr), :] = prob[:, h * LANES:(h + 1) * LANES]
        pnew[pl.ds(at_row(g), nr), :] = fresh

    def probs_of(g):
        return wide([pbuf[h, pl.ds(pl.multiple_of(g // per * 128, 128), 128), :] for h in range(s_max // LANES)])

    def mix(base, g, rhs, new):
        slot = lax.rem(base + g, RING)
        seq = lax.broadcasted_iota(jnp.int32, (hw, 128), 1) // heads - lax.rem(g, per) * CB
        for b in range(CB):
            o = lax.dot_general(wide([vbuf[slot, b, h] for h in range(s_max // LANES)]), rhs, (((1,), (1,)), ((), ())),
                                preferred_element_type=F32)
            new = jnp.where(seq == b, o, new)
        return new

    def refill(ci, i):
        @pl.when(ci + RING < total_chunks)
        def _():
            kv_start(ci + RING, i)

    def attention_pair(s, layer, g, tail):
        base = (layer * STREAMS + s) * nchunk
        kv_wait(base + g, 1)
        kv_wait(base + g + 1, 1)
        if not tail:
            kv_wait(base + g + 2, 0)
            kv_wait(base + g + 3, 0)
        sc = sbuf[...]
        rhs = probs_of(g)
        new = tmix[g // per]
        pa = softmax_of(s, g + 1, sc)
        if not tail:
            sc = scores_of(base, g + 2)
        new = mix(base, g, rhs, new)
        keep_probs(g + 1, *pa)
        rhs = probs_of(g + 1)
        if not tail:
            pa = softmax_of(s, g + 2, sc)
            sc = scores_of(base, g + 3)
        new = mix(base, g + 1, rhs, new)
        tmix[g // per] = new
        if not tail:
            keep_probs(g + 2, *pa)
            sbuf[...] = sc
        for k in range(2):
            refill(base + g + k, 1)
            if not tail:
                refill(base + g + 2 + k, 0)

    def attention(s, layer, lo, hi):
        base = (layer * STREAMS + s) * nchunk
        if lo == 0:
            kv_wait(base, 0)
            kv_wait(base + 1, 0)
            pa = softmax_of(s, 0, scores_of(base, 0))
            sbuf[...] = scores_of(base, 1)
            keep_probs(0, *pa)
            refill(base, 0)
            refill(base + 1, 0)

        def body(p, carry):
            attention_pair(s, layer, 2 * p, False)
            return carry

        stop = min(hi, nchunk - 2) // 2
        if stop - lo // 2 > 1:
            lax.fori_loop(lo // 2, stop, body, 0)
        elif stop > lo // 2:
            attention_pair(s, layer, lo, False)
        if hi == nchunk:
            attention_pair(s, layer, nchunk - 2, True)

    def att_copy(s, i):
        src, dev = ((0, dev_p), (0, dev_x), (2, dev_p))[i]
        return rcopy(att.at[s, src], att.at[s, i + 1], at_ssem.at[s, i], at_rsem.at[s, i], dev)

    def att_send(s):
        hr = heads * rows
        sel = (lax.broadcasted_iota(jnp.int32, (rows, hr), 1) // heads
               == lax.broadcasted_iota(jnp.int32, (rows, hr), 0)).astype(F32).astype(BF16)
        pe = jnp.where(head_mask(hr), jnp.broadcast_to(pnew[:, 0:1], (hr, hw)), 0.0).astype(BF16)
        o = jnp.dot(sel, pe, preferred_element_type=F32) * vfull[rsl(s), :hw]
        feat = lax.broadcasted_iota(jnp.int32, (hw, 128), 0)
        lane = lax.rem(lax.broadcasted_iota(jnp.int32, (hw, 128), 1), heads)
        own = (feat >= lane * hd) & (feat < lane * hd + hd)
        for half in range(hr // 128):
            t = jnp.where(own, tmix[half], 0.0)
            high = t.astype(BF16)
            low = (t - high.astype(F32)).astype(BF16)
            pick = sel[:, half * 128:(half + 1) * 128]
            for part in (high, low):
                o = o + lax.dot_general(pick, part, (((1,), (1,)), ((), ())), preferred_element_type=F32)
        att[s, 0] = o.astype(BF16)
        att_copy(s, 1).start()
        att_copy(s, 0).start()

    def att_relay(s):
        att_copy(s, 1).wait_recv()
        att_copy(s, 2).start()

    def y_copy(s, which):
        return rcopy(ysend.at[which, s], yrecv.at[which, s], y_ssem.at[which, s], y_rsem.at[which, s], dev_y)

    def out_proj(s):
        att_copy(s, 0).wait()
        att_copy(s, 1).wait_send()
        att_copy(s, 2).wait()
        res = None
        for i, owner in enumerate((r, partner, xpeer, diag)):
            off = pl.multiple_of(owner * hw, 16)
            t = jnp.dot(att[s, i], wide([wo[n, pl.ds(off, hw), :] for n in range(nt)]), preferred_element_type=F32)
            res = t if res is None else res + t
        ysend[0, s] = res.astype(BF16)
        y_copy(s, 0).start()

    def residual(s, which, bias):
        y_copy(s, which).wait()
        both = ysend[which, s].astype(F32) + yrecv[which, s].astype(F32)
        new = (state[rsl(s), :].astype(F32) + (both + bias.astype(F32))).astype(BF16)
        return new

    def fd_copy(s, j):
        return rcopy(fd_send.at[s, j], fd_recv.at[s, j], fd_ssem.at[s, j], fd_rsem.at[s, j], dev_p)

    def fx_copy(s, j):
        return rcopy(fx_send.at[s, j], fx_recv.at[s, j], fx_ssem.at[s, j], fx_rsem.at[s, j], dev_x)

    def u_copy(s, j, owner):
        return rcopy(u_buf.at[s, owner, j], u_buf.at[s, owner, j], u_ssem.at[s, j], u_rsem.at[s, j], dev_p)

    def fc1_part(s):
        yv = normed(s)

        def columns(owner, j):
            first = owner * (ff_half // LANES) + j * ct
            return jnp.dot(yv, wide([wf1[first + t] for t in range(ct)]), preferred_element_type=F32)

        for j in range(nj):
            res = columns(1 - core, j).astype(BF16)
            for t in range(ct):
                fd_send[s, j, t] = res[:, t * LANES:(t + 1) * LANES]
            fd_copy(s, j).start()
            f_mine[s, j] = columns(core, j)

    def fc1_forward(s, lo, hi):
        def body(j, carry):
            fd_copy(s, j).wait()
            for t in range(ct):
                fx_send[s, j, t] = (f_mine[s, j, :, t * LANES:(t + 1) * LANES] + fd_recv[s, j, t].astype(F32)).astype(BF16)
            fx_copy(s, j).start()
            return carry

        lax.fori_loop(lo, hi, body, 0)

    def fc2_add(s, j, owner):
        off = pl.multiple_of(owner * ff_half + j * CW, 128)
        u = wide([u_buf[s, owner, j, t] for t in range(ct)])
        acc[s] += jnp.dot(u, wide([wf2[n, pl.ds(off, CW), :] for n in range(nt)]), preferred_element_type=F32)

    def mlp(s, layer, lo, hi):
        if lo == 0:
            acc[s] = jnp.zeros(acc.shape[1:], F32)

        def body(j, carry):
            fx_copy(s, j).wait()
            off = pl.multiple_of(core * ff_half + j * CW, 128)
            bias = bf1_ref[layer:layer + 1, pl.ds(off, CW)].astype(F32)
            for t in range(ct):
                u = (fx_send[s, j, t].astype(F32) + fx_recv[s, j, t].astype(F32)) + bias[:, t * LANES:(t + 1) * LANES]
                u = u.astype(BF16)
                u_buf[s, core, j, t] = jnp.maximum(u, jnp.zeros_like(u))
            u_copy(s, j, core).start()
            fc2_add(s, j, core)

            @pl.when(j > 0)
            def _():
                u_copy(s, j - 1, 1 - core).wait_recv()
                fc2_add(s, j - 1, 1 - core)
            return carry

        lax.fori_loop(lo, hi, body, 0)
        if hi == nj:
            u_copy(s, nj - 1, 1 - core).wait_recv()
            fc2_add(s, nj - 1, 1 - core)

            def drain(j, carry):
                u_copy(s, j, core).wait_send()
                return carry

            lax.fori_loop(0, nj, drain, 0)
            ysend[1, s] = acc[s].astype(BF16)
            y_copy(s, 1).start()

    def kv_out(layer):
        kt_ref[layer] = kfull[...].T[:hw, :].astype(BF16)
        vt_ref[layer] = vfull[...].T[:hw, :].astype(BF16)

    def gain_ph(s, which, layer):
        g, b = (g1_ref, c1_ref) if which == 0 else (g2_ref, c2_ref)
        norm(s, which, g[layer:layer + 1, :], b[layer:layer + 1, :])

    def mid_ph(s, layer):
        new = residual(s, 0, bo_ref[layer:layer + 1, :])
        state[rsl(s), :] = new
        stats_send(s, 1, new.astype(F32))

    def end_ph(s, layer):
        new = residual(s, 1, bf2_ref[layer:layer + 1, :])
        if layer == layers - 1:
            out_ref[rsl(s), :] = new
        else:
            state[rsl(s), :] = new
            stats_send(s, 0, new.astype(F32))

    kfull[...] = jnp.zeros_like(kfull)
    vfull[...] = jnp.zeros_like(vfull)
    pbuf[...] = jnp.zeros_like(pbuf)
    tmix[...] = jnp.zeros_like(tmix)
    state[...] = hid_ref[...]
    stats_send(0, 0, state[rsl(0), :].astype(F32))
    stats_send(1, 0, state[rsl(1), :].astype(F32))
    w_wait("qkv", 0)
    gain_ph(0, 0, 0)
    qkv_part(0, 0)
    gain_ph(1, 0, 0)
    qkv_part(1, 0)
    qkv_forward(0)
    qkv_part(0, 1)
    qkv_forward(1)
    qkv_part(1, 1)
    w_start("qkv", 1)
    w_start("o", 0)
    w_start("f1", 0)
    w_start("f2", 0)
    qkv_finish(0, 0)
    attention(0, 0, 0, nchunk)
    att_send(0)
    q4 = nchunk // 4
    for layer in range(layers):
        last = layer == layers - 1
        qkv_finish(1, layer)
        attention(1, layer, 0, q4)
        att_relay(0)
        attention(1, layer, q4, 2 * q4)
        w_wait("o", layer)
        out_proj(0)
        attention(1, layer, 2 * q4, 3 * q4)
        kv_out(layer)
        mid_ph(0, layer)
        attention(1, layer, 3 * q4, nchunk)
        att_send(1)
        gain_ph(0, 1, layer)
        w_wait("f1", layer)
        fc1_part(0)
        fc1_forward(0, 0, nj)
        att_relay(1)
        w_wait("f2", layer)
        mlp(0, layer, 0, 1)
        out_proj(1)
        w_start("o", layer + 1)
        mlp(0, layer, 1, 3)
        mid_ph(1, layer)
        mlp(0, layer, 3, nj)
        gain_ph(1, 1, layer)
        fc1_part(1)
        w_start("f1", layer + 1)
        fc1_forward(1, 0, 2)
        end_ph(0, layer)
        fc1_forward(1, 2, nj)
        if not last:
            w_wait("qkv", layer + 1)
            gain_ph(0, 0, layer + 1)
            qkv_part(0, 0)
            qkv_forward(0)
            qkv_part(0, 1)
        mlp(1, layer, 0, nj)
        w_start("f2", layer + 1)
        if not last:
            qkv_finish(0, layer + 1)
            attention(0, layer + 1, 0, q4)
            end_ph(1, layer)
            attention(0, layer + 1, q4, 2 * q4)
            gain_ph(1, 0, layer + 1)
            qkv_part(1, 0)
            qkv_part(1, 1)
            w_start("qkv", layer + 2)
            qkv_forward(1)
            attention(0, layer + 1, 2 * q4, nchunk)
            att_send(0)
        else:
            end_ph(1, layer)


def finish(a_ref, b_ref, c_ref, x_ref, y_ref, z_ref):
    x_ref[...] = a_ref[...]
    y_ref[...] = b_ref[...]
    z_ref[...] = c_ref[...]


def solution(mesh):
    act_spec = P("dp", "row")
    cache_spec = P(None, "dp", ("col", "row"), None, None)
    fresh_spec = P(None, "dp", ("col", "row"), None)
    in_weight = P(None, "row", "col")
    out_weight = P(None, "col", "row")
    col_vec = P(None, "col")
    row_vec = P(None, "row")
    in_specs = (act_spec, P("dp"), cache_spec, cache_spec, row_vec, row_vec,
                in_weight, col_vec, in_weight, col_vec, in_weight, col_vec,
                out_weight, row_vec, row_vec, row_vec, in_weight, col_vec, out_weight, row_vec)

    def local_step(hidden, cache_len, k_cache, v_cache, ln1_g, ln1_b, w_q, b_q, w_k, b_k, w_v, b_v,
                   w_o, b_o, ln2_g, ln2_b, w_fc1, b_fc1, w_fc2, b_fc2):
        layers, batch, heads, s_max, hd = k_cache.shape
        dm = hidden.shape[1]
        hw = heads * hd
        ff = w_fc1.shape[2]
        rows = batch // STREAMS
        nj = ff // 2 // CW
        nt = dm // LANES
        ct = CW // LANES
        kt = k_cache.transpose(0, 1, 2, 4, 3).reshape(layers, batch, hw, s_max)
        vt = v_cache.transpose(0, 1, 2, 4, 3).reshape(layers, batch, hw, s_max)
        vm = pl.BlockSpec(memory_space=pltpu.VMEM)
        hb = pl.BlockSpec(memory_space=pl.ANY)
        sm = pl.BlockSpec(memory_space=pltpu.SMEM)
        hr = heads * rows
        V = pltpu.VMEM
        D = pltpu.SemaphoreType.DMA
        scratch = [
            V((RING, CB, s_max // LANES, hw, LANES), BF16), V((RING, CB, s_max // LANES, hw, LANES), BF16),
            V((2, 3 * nt, dm, LANES), BF16), V((nt, w_o.shape[1], LANES), BF16),
            V((ff // LANES, dm, LANES), BF16), V((nt, ff, LANES), BF16),
            V((batch, dm), BF16), V((nt, batch, LANES), BF16),
            V((2, STREAMS, 8, 2 * rows), F32), V((2, STREAMS, 3, 8, 2 * rows), F32),
            V((STREAMS, 2, rows, 3 * hw), BF16), V((STREAMS, 2, rows, 3 * hw), BF16), V((STREAMS, 2, rows, 3 * hw), F32),
            V((STREAMS, rows, 3 * hw), BF16), V((STREAMS, rows, 3 * hw), BF16),
            V((hr, hw), BF16), V((hr, 128), F32), V((CB * heads, s_max), F32), V((s_max // LANES, hr, LANES), BF16), V((hr, 128), F32),
            V((hr // 128, hw, 128), F32),
            V((STREAMS, 4, rows, hw), BF16), V((batch, 384), F32), V((batch, 384), F32),
            V((2, STREAMS, rows, dm), BF16), V((2, STREAMS, rows, dm), BF16), V((STREAMS, rows, dm), F32),
            V((STREAMS, nj, ct, rows, LANES), BF16), V((STREAMS, nj, ct, rows, LANES), BF16), V((STREAMS, nj, rows, CW), F32),
            V((STREAMS, nj, ct, rows, LANES), BF16), V((STREAMS, nj, ct, rows, LANES), BF16),
            V((STREAMS, 2, nj, ct, rows, LANES), BF16),
            D((2, s_max // LANES, RING)), D((3, 2 * nt)), D((nt,)), D((ff // LANES,)), D((nt,)), D((2, STREAMS, 3)), D((2, STREAMS, 3)),
            D((STREAMS, 2)), D((STREAMS, 2)), D((STREAMS,)), D((STREAMS,)),
            D((STREAMS, 3)), D((STREAMS, 3)), D((2, STREAMS)), D((2, STREAMS)),
            D((STREAMS, nj)), D((STREAMS, nj)), D((STREAMS, nj)), D((STREAMS, nj)), D((STREAMS, nj)), D((STREAMS, nj)),
        ]
        out, kn, vn = pl.pallas_call(
            functools.partial(fused, (layers, batch, dm, hw, heads, s_max, ff)),
            out_shape=(jax.ShapeDtypeStruct((batch, dm), BF16),
                       jax.ShapeDtypeStruct((layers, hw, batch), BF16),
                       jax.ShapeDtypeStruct((layers, hw, batch), BF16)),
            in_specs=[vm, sm, hb, hb, vm, vm, hb, vm, hb, vm, hb, vm, hb, vm, vm, vm, hb, vm, hb, vm],
            out_specs=(vm, vm, vm),
            scratch_shapes=scratch,
            compiler_params=pltpu.CompilerParams(collective_id=0, has_side_effects=True,
                                                 vmem_limit_bytes=67043328),
        )(hidden, cache_len, kt, vt, ln1_g, ln1_b, w_q, b_q, w_k, b_k, w_v, b_v,
          w_o, b_o, ln2_g, ln2_b, w_fc1, b_fc1, w_fc2, b_fc2)
        out, kn, vn = pl.pallas_call(
            finish, out_shape=tuple(jax.ShapeDtypeStruct(a.shape, a.dtype) for a in (out, kn, vn)),
            in_specs=[vm] * 3, out_specs=(vm,) * 3)(out, kn, vn)
        kn = kn.reshape(layers, heads, hd, batch).transpose(0, 3, 1, 2)
        vn = vn.reshape(layers, heads, hd, batch).transpose(0, 3, 1, 2)
        return out, kn, vn

    return jax.shard_map(local_step, mesh=mesh, in_specs=in_specs,
                         out_specs=(act_spec, fresh_spec, fresh_spec), check_vma=False)
```

```python
import functools

import jax
import jax.numpy as jnp
from jax import lax
from jax.experimental import pallas as pl
from jax.experimental.pallas import tpu as pltpu
from jax.sharding import PartitionSpec as P

EPS_LN = 1e-5
F32 = jnp.float32
BF16 = jnp.bfloat16
STREAMS = 2
RING = 12
CB = 8
CW = 512
MESH = pl.DeviceIdType.MESH
LANES = 128


def wide(tiles):
    return jnp.concatenate(tiles, axis=1)


def fused(dims, hid_hbm, len_hbm, k_hbm, v_hbm, g1_hbm, c1_hbm, wq_hbm, bq_hbm, wk_hbm, bk_hbm, wv_hbm, bv_hbm,
          wo_hbm, bo_hbm, g2_hbm, c2_hbm, f1_hbm, bf1_hbm, f2_hbm, bf2_hbm,
          out_ref, kt_ref, vt_ref,
          kbuf, vbuf, wqkv, wo, wf1, wf2,
          len_ref, g1_ref, c1_ref, bq_ref, bk_ref, bv_ref, bo_ref, g2_ref, c2_ref, bf1_ref, bf2_ref,
          state, ynorm, st_send, st_recv,
          qd_send, qd_recv, kd_send, kd_recv, q_mine, qx_send, qx_recv, kx_send, kx_recv,
          qblk, snew, sbuf, pbuf, pnew, tmix, att, kfull, vfull,
          ysend, yrecv, acc,
          fd_send, fd_recv, f_mine, fx_send, fx_recv, u_buf,
          in_sem, kv_sem, wq_sem, wo_sem, f1_sem, f2_sem, st_ssem, st_rsem, qd_ssem, qd_rsem, qx_ssem, qx_rsem,
          at_ssem, at_rsem, y_ssem, y_rsem, fd_ssem, fd_rsem, fx_ssem, fx_rsem, u_ssem, u_rsem):
    layers, batch, dm, hw, heads, s_max, ff = dims
    hd = hw // heads
    d_total = dm * 4
    rows = batch // STREAMS
    nchunk = rows // CB
    total_chunks = layers * STREAMS * nchunk
    ff_half = ff // 2
    nt = dm // LANES
    ct = CW // LANES
    nj = ff_half // CW

    r = lax.axis_index("row")
    c = lax.axis_index("col")
    core = lax.rem(r, 2)
    chip = r // 2
    partner = r + 1 - 2 * core
    xpeer = lax.rem(r + 2, 4)
    diag = lax.rem(partner + 2, 4)
    dev_p = {"row": partner}
    dev_x = {"row": xpeer}
    dev_d = {"row": diag}
    dev_y = {"col": 1 - c}

    def rcopy(src, dst, ssem, rsem, dev):
        return pltpu.make_async_remote_copy(src_ref=src, dst_ref=dst, send_sem=ssem, recv_sem=rsem,
                                            device_id=dev, device_id_type=MESH)

    def kv_copies(ci, i):
        layer = ci // (STREAMS * nchunk)
        first = lax.rem(ci, STREAMS * nchunk) * CB
        slot = lax.rem(ci, RING)
        src, dst = ((k_hbm, kbuf), (v_hbm, vbuf))[i]
        return [pltpu.make_async_copy(src.at[layer, pl.ds(first, CB), :, pl.ds(h * LANES, LANES)], dst.at[slot, :, h],
                                      kv_sem.at[i, h, slot]) for h in range(s_max // LANES)]

    def kv_start(ci, i):
        for cp in kv_copies(ci, i):
            cp.start()

    def kv_wait(ci, i):
        for cp in kv_copies(ci, i):
            cp.wait()

    def w_each(name, layer, act):
        def run(src, dst, sems, tiles):
            def body(t, carry):
                cp = pltpu.make_async_copy(src.at[layer, :, pl.ds(pl.multiple_of(t * LANES, LANES), LANES)], dst(t), sems(t))
                cp.start() if act else cp.wait()
                return carry
            lax.fori_loop(0, tiles, body, 0)

        if name == "qkv":
            for i, w in enumerate((wq_hbm, wk_hbm, wv_hbm)):
                run(w, lambda t, i=i: wqkv.at[t // nt, i * nt + lax.rem(t, nt)], lambda t, i=i: wq_sem.at[i, t], 2 * nt)
        elif name == "o":
            run(wo_hbm, lambda t: wo.at[t], lambda t: wo_sem.at[t], nt)
        elif name == "f1":
            run(f1_hbm, lambda t: wf1.at[t], lambda t: f1_sem.at[t], ff // LANES)
        else:
            run(f2_hbm, lambda t: wf2.at[t], lambda t: f2_sem.at[t], nt)

    def w_start(name, layer):
        if layer < layers:
            w_each(name, layer, True)

    def w_wait(name, layer):
        w_each(name, layer, False)

    small = [pltpu.make_async_copy(a, b, in_sem.at[n]) for n, (a, b) in enumerate((
        (hid_hbm, state), (len_hbm, len_ref), (g1_hbm, g1_ref), (c1_hbm, c1_ref), (bq_hbm, bq_ref), (bk_hbm, bk_ref),
        (bv_hbm, bv_ref), (bo_hbm, bo_ref), (g2_hbm, g2_ref), (c2_hbm, c2_ref), (bf1_hbm, bf1_ref), (bf2_hbm, bf2_ref)))]
    small[0].start()
    barrier = pltpu.get_barrier_semaphore()
    for dev in (dev_p, dev_x, dev_d, dev_y):
        pl.semaphore_signal(barrier, inc=1, device_id=dev, device_id_type=MESH)
    for cp in small[1:]:
        cp.start()
    w_start("qkv", 0)

    def prime(ci, carry):
        kv_start(ci, 0)
        kv_start(ci, 1)
        return carry

    def rsl(s):
        return pl.ds(s * rows, rows)

    def stat_copies(s, which):
        return [rcopy(st_send.at[which, s], st_recv.at[which, s, i], st_ssem.at[which, s, i], st_rsem.at[which, s, i], dev)
                for i, dev in enumerate((dev_p, dev_x, dev_d))]

    def stats_send(s, which, xv):
        p1 = xv[:, 0:128]
        p2 = p1 * p1
        for i in range(1, dm // 128):
            t = xv[:, i * 128:(i + 1) * 128]
            p1 = p1 + t
            p2 = p2 + t * t
        both = jnp.concatenate([p1, p2], axis=0)
        row = jnp.sum(both.T, axis=0, keepdims=True)
        st_send[which, s] = jnp.broadcast_to(row, (8, 2 * rows))
        for cp in stat_copies(s, which):
            cp.start()

    def norm(s, which, gain, shift):
        for cp in stat_copies(s, which):
            cp.wait()
        row = ((st_send[which, s, 0:1, :] + st_recv[which, s, 0, 0:1, :])
               + (st_recv[which, s, 1, 0:1, :] + st_recv[which, s, 2, 0:1, :]))
        n2 = 2 * rows
        eye = lax.broadcasted_iota(jnp.int32, (n2, n2), 0) == lax.broadcasted_iota(jnp.int32, (n2, n2), 1)
        col = jnp.sum(jnp.where(eye, jnp.broadcast_to(row, (n2, n2)), 0.0), axis=1, keepdims=True)
        mean = col[0:rows] * (1.0 / d_total)
        var = col[rows:] * (1.0 / d_total) - mean * mean
        rstd = lax.rsqrt(var + EPS_LN)
        xv = state[rsl(s), :].astype(F32)
        y = ((xv - mean) * rstd * gain.astype(F32) + shift.astype(F32)).astype(BF16)
        for t in range(nt):
            ynorm[t, rsl(s), :] = y[:, t * LANES:(t + 1) * LANES]

    def normed(s):
        return wide([ynorm[t, rsl(s), :] for t in range(nt)])

    def qd_copy(s, i, m):
        src, dst = ((qd_send, qd_recv), (kd_send, kd_recv))[m]
        return rcopy(src.at[s, i], dst.at[s, i], qd_ssem.at[s, i, m], qd_rsem.at[s, i, m], dev_p)

    def qx_copy(s, m):
        src, dst = ((qx_send, qx_recv), (kx_send, kx_recv))[m]
        return rcopy(src.at[s], dst.at[s], qx_ssem.at[s, m], qx_rsem.at[s, m], dev_x)

    def qkv_part(s, i):
        target = 1 - chip if i == 0 else chip
        res = jnp.dot(normed(s), wide([wqkv[target, t] for t in range(3 * nt)]), preferred_element_type=F32)
        for m in range(3):
            low, high = res[:, 2 * m * hw:(2 * m + 1) * hw], res[:, (2 * m + 1) * hw:(2 * m + 2) * hw]
            q_mine[s, i, :, m * hw:(m + 1) * hw] = jnp.where(core == 0, low, high)
            away = jnp.where(core == 0, high, low).astype(BF16)
            if m == 0:
                qd_send[s, i] = away
            else:
                kd_send[s, i, :, (m - 1) * hw:m * hw] = away
        qd_copy(s, i, 0).start()
        qd_copy(s, i, 1).start()

    def qkv_forward(s):
        qd_copy(s, 0, 0).wait()
        qx_send[s] = (q_mine[s, 0, :, 0:hw] + qd_recv[s, 0].astype(F32)).astype(BF16)
        qx_copy(s, 0).start()
        qd_copy(s, 0, 1).wait()
        kx_send[s] = (q_mine[s, 0, :, hw:3 * hw] + kd_recv[s, 0].astype(F32)).astype(BF16)
        qx_copy(s, 1).start()

    def own_bias(b_ref, layer):
        b = b_ref[layer:layer + 1, :].astype(F32)
        parts = [b[:, i * hw:(i + 1) * hw] for i in range(4)]
        return jnp.where(r == 0, parts[0], jnp.where(r == 1, parts[1], jnp.where(r == 2, parts[2], parts[3])))

    def expand_mat():
        hr = heads * rows
        return (lax.broadcasted_iota(jnp.int32, (hr, rows), 0) // heads
                == lax.broadcasted_iota(jnp.int32, (hr, rows), 1)).astype(F32).astype(BF16)

    def head_mask(n):
        row = lax.rem(lax.broadcasted_iota(jnp.int32, (n, hw), 0), heads)
        lane = lax.broadcasted_iota(jnp.int32, (n, hw), 1)
        return (lane >= row * hd) & (lane < row * hd + hd)

    def q_finish(s, layer):
        qd_copy(s, 1, 0).wait()
        qx_copy(s, 0).wait()
        tot = (q_mine[s, 1, :, 0:hw] + qd_recv[s, 1].astype(F32)) + qx_recv[s].astype(F32)
        q = ((tot + own_bias(bq_ref, layer)) * (hd ** -0.5)).astype(BF16)
        qblk[...] = jnp.where(head_mask(heads * rows), jnp.dot(expand_mat(), q, preferred_element_type=F32), 0.0).astype(BF16)

    def kv_finish(s, layer):
        qd_copy(s, 1, 1).wait()
        qx_copy(s, 1).wait()
        tot = (q_mine[s, 1, :, hw:3 * hw] + kd_recv[s, 1].astype(F32)) + kx_recv[s].astype(F32)
        k = (tot[:, 0:hw] + own_bias(bk_ref, layer)).astype(BF16)
        v = (tot[:, hw:2 * hw] + own_bias(bv_ref, layer)).astype(BF16)
        kfull[rsl(s), :hw] = k.astype(F32)
        vfull[rsl(s), :hw] = v.astype(F32)
        ke = jnp.dot(expand_mat(), k, preferred_element_type=F32)
        snew[...] = jnp.broadcast_to(jnp.sum(qblk[...].astype(F32) * ke, axis=1, keepdims=True), snew.shape)

    nr = CB * heads
    per = 128 // nr
    upper = lax.broadcasted_iota(jnp.int32, (8, 1), 0) < heads

    pos = lax.broadcasted_iota(jnp.int32, (nr, s_max), 1)

    def at_row(g):
        return pl.multiple_of(g * nr, nr)

    def scores_of(base, g):
        slot = lax.rem(base + g, RING)
        out = []
        for t in range(nr // 16):
            lhs = qblk[pl.ds(pl.multiple_of(at_row(g) + t * 16, 16), 16), :]
            d = [jnp.dot(lhs, wide([kbuf[slot, t * 4 + i, h] for h in range(s_max // LANES)]), preferred_element_type=F32)
                 for i in range(4)]
            out.append(jnp.where(upper, d[0][0:8], d[1][0:8]))
            out.append(jnp.where(upper, d[2][8:16], d[3][8:16]))
        return jnp.concatenate(out, axis=0)

    def softmax_of(s, g, sc):
        lens = []
        for i in range(0, CB, 2):
            b = s * rows + g * CB + i
            lens.append(jnp.where(upper, len_ref[b], len_ref[b + 1]))
        sc = jnp.where(pos < jnp.concatenate(lens, axis=0), sc, -jnp.inf)
        sn = snew[pl.ds(at_row(g), nr), 0:1]
        peak = jnp.maximum(jnp.max(sc, axis=1, keepdims=True), sn)
        e = jnp.exp(sc - peak)
        en = jnp.exp(sn - peak)
        inv = 1.0 / (jnp.sum(e, axis=1, keepdims=True) + en)
        return (e * inv).astype(BF16), jnp.broadcast_to(en * inv, (nr, LANES))

    def keep_probs(g, prob, fresh):
        for h in range(s_max // LANES):
            pbuf[h, pl.ds(at_row(g), nr), :] = prob[:, h * LANES:(h + 1) * LANES]
        pnew[pl.ds(at_row(g), nr), :] = fresh

    def probs_of(g):
        return wide([pbuf[h, pl.ds(pl.multiple_of(g // per * 128, 128), 128), :] for h in range(s_max // LANES)])

    def mix(base, g, rhs, new):
        slot = lax.rem(base + g, RING)
        seq = lax.broadcasted_iota(jnp.int32, (hw, 128), 1) // heads - lax.rem(g, per) * CB
        for b in range(CB):
            o = lax.dot_general(wide([vbuf[slot, b, h] for h in range(s_max // LANES)]), rhs, (((1,), (1,)), ((), ())),
                                preferred_element_type=F32)
            new = jnp.where(seq == b, o, new)
        return new

    def refill(ci, i):
        @pl.when(ci + RING < total_chunks)
        def _():
            kv_start(ci + RING, i)

    def attention_pair(s, layer, g, tail):
        base = (layer * STREAMS + s) * nchunk
        kv_wait(base + g, 1)
        kv_wait(base + g + 1, 1)
        if not tail:
            kv_wait(base + g + 2, 0)
            kv_wait(base + g + 3, 0)
        sc = sbuf[...]
        rhs = probs_of(g)
        new = tmix[g // per]
        pa = softmax_of(s, g + 1, sc)
        if not tail:
            sc = scores_of(base, g + 2)
        new = mix(base, g, rhs, new)
        keep_probs(g + 1, *pa)
        rhs = probs_of(g + 1)
        if not tail:
            pa = softmax_of(s, g + 2, sc)
            sc = scores_of(base, g + 3)
        new = mix(base, g + 1, rhs, new)
        tmix[g // per] = new
        if not tail:
            keep_probs(g + 2, *pa)
            sbuf[...] = sc
        for k in range(2):
            refill(base + g + k, 1)
            if not tail:
                refill(base + g + 2 + k, 0)

    def attention(s, layer, lo, hi):
        base = (layer * STREAMS + s) * nchunk
        if lo == 0:
            kv_wait(base, 0)
            kv_wait(base + 1, 0)
            first = scores_of(base, 0)
            second = scores_of(base, 1)
            kv_finish(s, layer)
            pa = softmax_of(s, 0, first)
            sbuf[...] = second
            keep_probs(0, *pa)
            refill(base, 0)
            refill(base + 1, 0)

        def body(p, carry):
            attention_pair(s, layer, 2 * p, False)
            return carry

        stop = min(hi, nchunk - 2) // 2
        if stop - lo // 2 > 1:
            lax.fori_loop(lo // 2, stop, body, 0)
        elif stop > lo // 2:
            attention_pair(s, layer, lo, False)
        if hi == nchunk:
            attention_pair(s, layer, nchunk - 2, True)

    hrow = LANES // heads

    def att_copies(s, half):
        return [rcopy(att.at[s, 0, half], att.at[s, i + 1, half], at_ssem.at[s, i, half], at_rsem.at[s, i, half], dev)
                for i, dev in enumerate((dev_p, dev_x, dev_d))]

    def att_send(s, half):
        sel = (lax.broadcasted_iota(jnp.int32, (hrow, LANES), 1) // heads
               == lax.broadcasted_iota(jnp.int32, (hrow, LANES), 0)).astype(F32).astype(BF16)
        fresh = jnp.broadcast_to(pnew[half * LANES:(half + 1) * LANES, 0:1], (LANES, hw))
        pe = jnp.where(head_mask(LANES), fresh, 0.0).astype(BF16)
        first = s * rows + half * hrow
        o = jnp.dot(sel, pe, preferred_element_type=F32) * vfull[first:first + hrow, :hw]
        feat = lax.broadcasted_iota(jnp.int32, (hw, LANES), 0)
        lane = lax.rem(lax.broadcasted_iota(jnp.int32, (hw, LANES), 1), heads)
        t = jnp.where((feat >= lane * hd) & (feat < lane * hd + hd), tmix[half], 0.0)
        high = t.astype(BF16)
        low = (t - high.astype(F32)).astype(BF16)
        for part in (high, low):
            o = o + lax.dot_general(sel, part, (((1,), (1,)), ((), ())), preferred_element_type=F32)
        att[s, 0, half] = o.astype(BF16)
        p, x, d = att_copies(s, half)
        x.start()
        d.start()
        p.start()

    def y_copy(s, which):
        return rcopy(ysend.at[which, s], yrecv.at[which, s], y_ssem.at[which, s], y_rsem.at[which, s], dev_y)

    def out_proj(s):
        for half in range(rows // hrow):
            for cp in att_copies(s, half):
                cp.wait()
        res = None
        for i, owner in enumerate((r, partner, xpeer, diag)):
            off = pl.multiple_of(owner * hw, 16)
            t = jnp.dot(jnp.concatenate([att[s, i, h] for h in range(rows // hrow)], axis=0), wide([wo[n, pl.ds(off, hw), :] for n in range(nt)]), preferred_element_type=F32)
            res = t if res is None else res + t
        ysend[0, s] = res.astype(BF16)
        y_copy(s, 0).start()

    def residual(s, which, bias):
        y_copy(s, which).wait()
        both = ysend[which, s].astype(F32) + yrecv[which, s].astype(F32)
        new = (state[rsl(s), :].astype(F32) + (both + bias.astype(F32))).astype(BF16)
        return new

    def fd_copy(s, j):
        return rcopy(fd_send.at[s, j], fd_recv.at[s, j], fd_ssem.at[s, j], fd_rsem.at[s, j], dev_p)

    def fx_copy(s, j):
        return rcopy(fx_send.at[s, j], fx_recv.at[s, j], fx_ssem.at[s, j], fx_rsem.at[s, j], dev_x)

    def u_copy(s, j, owner):
        return rcopy(u_buf.at[s, owner, j], u_buf.at[s, owner, j], u_ssem.at[s, j], u_rsem.at[s, j], dev_p)

    def fc1_part(s):
        yv = normed(s)

        def columns(owner, first, n):
            at = owner * (ff_half // LANES) + first
            return jnp.dot(yv, wide([wf1[at + t] for t in range(n)]), preferred_element_type=F32)

        tiles = ff_half // LANES
        res = columns(1 - core, 0, tiles).astype(BF16)
        for j in range(nj):
            for t in range(ct):
                fd_send[s, j, t] = res[:, (j * ct + t) * LANES:(j * ct + t + 1) * LANES]
            fd_copy(s, j).start()
        res = columns(core, 0, tiles)
        for j in range(nj):
            f_mine[s, j] = res[:, j * CW:(j + 1) * CW]

    def fc1_forward(s, lo, hi):
        def body(j, carry):
            fd_copy(s, j).wait()
            for t in range(ct):
                fx_send[s, j, t] = (f_mine[s, j, :, t * LANES:(t + 1) * LANES] + fd_recv[s, j, t].astype(F32)).astype(BF16)
            fx_copy(s, j).start()
            return carry

        lax.fori_loop(lo, hi, body, 0)

    def fc2_add(s, j, owner):
        off = pl.multiple_of(owner * ff_half + j * CW, 128)
        u = wide([u_buf[s, owner, j, t] for t in range(ct)])
        acc[s] += jnp.dot(u, wide([wf2[n, pl.ds(off, CW), :] for n in range(nt)]), preferred_element_type=F32)

    def mlp(s, layer, lo, hi):
        if lo == 0:
            acc[s] = jnp.zeros(acc.shape[1:], F32)

        def body(j, carry):
            fx_copy(s, j).wait()
            off = pl.multiple_of(core * ff_half + j * CW, 128)
            bias = bf1_ref[layer:layer + 1, pl.ds(off, CW)].astype(F32)
            for t in range(ct):
                u = (fx_send[s, j, t].astype(F32) + fx_recv[s, j, t].astype(F32)) + bias[:, t * LANES:(t + 1) * LANES]
                u = u.astype(BF16)
                u_buf[s, core, j, t] = jnp.maximum(u, jnp.zeros_like(u))
            u_copy(s, j, core).start()
            fc2_add(s, j, core)

            @pl.when(j > 0)
            def _():
                u_copy(s, j - 1, 1 - core).wait_recv()
                fc2_add(s, j - 1, 1 - core)
            return carry

        lax.fori_loop(lo, hi, body, 0)
        if hi == nj:
            u_copy(s, nj - 1, 1 - core).wait_recv()
            fc2_add(s, nj - 1, 1 - core)

            def drain(j, carry):
                u_copy(s, j, core).wait_send()
                return carry

            lax.fori_loop(0, nj, drain, 0)
            ysend[1, s] = acc[s].astype(BF16)
            y_copy(s, 1).start()

    def kv_out(layer):
        kt_ref[layer] = kfull[...].T[:hw, :].astype(BF16)
        vt_ref[layer] = vfull[...].T[:hw, :].astype(BF16)

    def gain_ph(s, which, layer):
        g, b = (g1_ref, c1_ref) if which == 0 else (g2_ref, c2_ref)
        norm(s, which, g[layer:layer + 1, :], b[layer:layer + 1, :])

    def mid_ph(s, layer):
        new = residual(s, 0, bo_ref[layer:layer + 1, :])
        state[rsl(s), :] = new
        stats_send(s, 1, new.astype(F32))

    def end_ph(s, layer):
        new = residual(s, 1, bf2_ref[layer:layer + 1, :])
        if layer == layers - 1:
            out_ref[rsl(s), :] = new
        else:
            state[rsl(s), :] = new
            stats_send(s, 0, new.astype(F32))

    small[0].wait()
    pl.semaphore_wait(barrier, 4)
    stats_send(0, 0, state[rsl(0), :].astype(F32))
    stats_send(1, 0, state[rsl(1), :].astype(F32))
    lax.fori_loop(0, RING, prime, 0)
    kfull[...] = jnp.zeros_like(kfull)
    vfull[...] = jnp.zeros_like(vfull)
    pbuf[...] = jnp.zeros_like(pbuf)
    tmix[...] = jnp.zeros_like(tmix)
    for cp in small[1:]:
        cp.wait()
    w_wait("qkv", 0)
    gain_ph(0, 0, 0)
    qkv_part(0, 0)
    gain_ph(1, 0, 0)
    qkv_part(1, 0)
    qkv_forward(0)
    qkv_part(0, 1)
    qkv_forward(1)
    qkv_part(1, 1)
    w_start("qkv", 1)
    w_start("o", 0)
    w_start("f1", 0)
    w_start("f2", 0)
    q_finish(0, 0)
    attention(0, 0, 0, nchunk // 2)
    att_send(0, 0)
    attention(0, 0, nchunk // 2, nchunk)
    att_send(0, 1)
    q4 = nchunk // 4
    for layer in range(layers):
        last = layer == layers - 1
        q_finish(1, layer)
        attention(1, layer, 0, q4)
        w_wait("o", layer)
        out_proj(0)
        attention(1, layer, q4, 2 * q4)
        att_send(1, 0)
        attention(1, layer, 2 * q4, 3 * q4)
        mid_ph(0, layer)
        attention(1, layer, 3 * q4, nchunk)
        att_send(1, 1)
        kv_out(layer)
        w_wait("f1", layer)
        gain_ph(0, 1, layer)
        fc1_part(0)
        fc1_forward(0, 0, 3)
        out_proj(1)
        w_start("o", layer + 1)
        w_wait("f2", layer)
        mlp(0, layer, 0, 1)
        mid_ph(1, layer)
        fc1_forward(0, 3, nj)
        mlp(0, layer, 1, 3)
        gain_ph(1, 1, layer)
        fc1_part(1)
        w_start("f1", layer + 1)
        fc1_forward(1, 0, 4)
        mlp(0, layer, 3, nj)
        mlp(1, layer, 0, 1)
        end_ph(0, layer)
        fc1_forward(1, 4, nj)
        mlp(1, layer, 1, 2)
        if not last:
            w_wait("qkv", layer + 1)
            gain_ph(0, 0, layer + 1)
            qkv_part(0, 0)
            qkv_part(0, 1)
            qkv_forward(0)
        mlp(1, layer, 2, nj)
        w_start("f2", layer + 1)
        if not last:
            q_finish(0, layer + 1)
            attention(0, layer + 1, 0, q4)
            attention(0, layer + 1, q4, 2 * q4)
            end_ph(1, layer)
            att_send(0, 0)
            attention(0, layer + 1, 2 * q4, 3 * q4)
            gain_ph(1, 0, layer + 1)
            qkv_part(1, 0)
            qkv_part(1, 1)
            w_start("qkv", layer + 2)
            qkv_forward(1)
            attention(0, layer + 1, 3 * q4, nchunk)
            att_send(0, 1)
        else:
            end_ph(1, layer)


def finish(a_ref, b_ref, c_ref, x_ref, y_ref, z_ref):
    x_ref[...] = a_ref[...]
    y_ref[...] = b_ref[...]
    z_ref[...] = c_ref[...]


def solution(mesh):
    act_spec = P("dp", "row")
    cache_spec = P(None, "dp", ("col", "row"), None, None)
    fresh_spec = P(None, "dp", ("col", "row"), None)
    in_weight = P(None, "row", "col")
    out_weight = P(None, "col", "row")
    col_vec = P(None, "col")
    row_vec = P(None, "row")
    in_specs = (act_spec, P("dp"), cache_spec, cache_spec, row_vec, row_vec,
                in_weight, col_vec, in_weight, col_vec, in_weight, col_vec,
                out_weight, row_vec, row_vec, row_vec, in_weight, col_vec, out_weight, row_vec)

    def local_step(hidden, cache_len, k_cache, v_cache, ln1_g, ln1_b, w_q, b_q, w_k, b_k, w_v, b_v,
                   w_o, b_o, ln2_g, ln2_b, w_fc1, b_fc1, w_fc2, b_fc2):
        layers, batch, heads, s_max, hd = k_cache.shape
        dm = hidden.shape[1]
        hw = heads * hd
        ff = w_fc1.shape[2]
        rows = batch // STREAMS
        nj = ff // 2 // CW
        nt = dm // LANES
        ct = CW // LANES
        kt = k_cache.transpose(0, 1, 2, 4, 3).reshape(layers, batch, hw, s_max)
        vt = v_cache.transpose(0, 1, 2, 4, 3).reshape(layers, batch, hw, s_max)
        vm = pl.BlockSpec(memory_space=pltpu.VMEM)
        hb = pl.BlockSpec(memory_space=pl.ANY)
        hr = heads * rows
        V = pltpu.VMEM
        D = pltpu.SemaphoreType.DMA
        scratch = [
            V((RING, CB, s_max // LANES, hw, LANES), BF16), V((RING, CB, s_max // LANES, hw, LANES), BF16),
            V((2, 3 * nt, dm, LANES), BF16), V((nt, w_o.shape[1], LANES), BF16),
            V((ff // LANES, dm, LANES), BF16), V((nt, ff, LANES), BF16),
            pltpu.SMEM((batch,), jnp.int32), V((layers, dm), BF16), V((layers, dm), BF16),
            V(b_q.shape, BF16), V(b_k.shape, BF16), V(b_v.shape, BF16), V(b_o.shape, BF16),
            V((layers, dm), BF16), V((layers, dm), BF16), V(b_fc1.shape, BF16), V(b_fc2.shape, BF16),
            V((batch, dm), BF16), V((nt, batch, LANES), BF16),
            V((2, STREAMS, 8, 2 * rows), F32), V((2, STREAMS, 3, 8, 2 * rows), F32),
            V((STREAMS, 2, rows, hw), BF16), V((STREAMS, 2, rows, hw), BF16), V((STREAMS, 2, rows, 2 * hw), BF16), V((STREAMS, 2, rows, 2 * hw), BF16),
            V((STREAMS, 2, rows, 3 * hw), F32),
            V((STREAMS, rows, hw), BF16), V((STREAMS, rows, hw), BF16), V((STREAMS, rows, 2 * hw), BF16), V((STREAMS, rows, 2 * hw), BF16),
            V((hr, hw), BF16), V((hr, 128), F32), V((CB * heads, s_max), F32), V((s_max // LANES, hr, LANES), BF16), V((hr, 128), F32),
            V((hr // 128, hw, 128), F32),
            V((STREAMS, 4, hr // LANES, LANES // heads, hw), BF16), V((batch, 384), F32), V((batch, 384), F32),
            V((2, STREAMS, rows, dm), BF16), V((2, STREAMS, rows, dm), BF16), V((STREAMS, rows, dm), F32),
            V((STREAMS, nj, ct, rows, LANES), BF16), V((STREAMS, nj, ct, rows, LANES), BF16), V((STREAMS, nj, rows, CW), F32),
            V((STREAMS, nj, ct, rows, LANES), BF16), V((STREAMS, nj, ct, rows, LANES), BF16),
            V((STREAMS, 2, nj, ct, rows, LANES), BF16),
            D((12,)), D((2, s_max // LANES, RING)), D((3, 2 * nt)), D((nt,)), D((ff // LANES,)), D((nt,)), D((2, STREAMS, 3)), D((2, STREAMS, 3)),
            D((STREAMS, 2, 2)), D((STREAMS, 2, 2)), D((STREAMS, 2)), D((STREAMS, 2)),
            D((STREAMS, 3, hr // LANES)), D((STREAMS, 3, hr // LANES)), D((2, STREAMS)), D((2, STREAMS)),
            D((STREAMS, nj)), D((STREAMS, nj)), D((STREAMS, nj)), D((STREAMS, nj)), D((STREAMS, nj)), D((STREAMS, nj)),
        ]
        out, kn, vn = pl.pallas_call(
            functools.partial(fused, (layers, batch, dm, hw, heads, s_max, ff)),
            out_shape=(jax.ShapeDtypeStruct((batch, dm), BF16),
                       jax.ShapeDtypeStruct((layers, hw, batch), BF16),
                       jax.ShapeDtypeStruct((layers, hw, batch), BF16)),
            in_specs=[hb] * 20,
            out_specs=(vm, vm, vm),
            scratch_shapes=scratch,
            compiler_params=pltpu.CompilerParams(collective_id=0, has_side_effects=True,
                                                 vmem_limit_bytes=67043328),
        )(hidden, cache_len, kt, vt, ln1_g, ln1_b, w_q, b_q, w_k, b_k, w_v, b_v,
          w_o, b_o, ln2_g, ln2_b, w_fc1, b_fc1, w_fc2, b_fc2)
        out, kn, vn = pl.pallas_call(
            finish, out_shape=tuple(jax.ShapeDtypeStruct(a.shape, a.dtype) for a in (out, kn, vn)),
            in_specs=[vm] * 3, out_specs=(vm,) * 3)(out, kn, vn)
        kn = kn.reshape(layers, heads, hd, batch).transpose(0, 3, 1, 2)
        vn = vn.reshape(layers, heads, hd, batch).transpose(0, 3, 1, 2)
        return out, kn, vn

    return jax.shard_map(local_step, mesh=mesh, in_specs=in_specs,
                         out_specs=(act_spec, fresh_spec, fresh_spec), check_vma=False)
```

```python
import functools

import jax
import jax.numpy as jnp
from jax import lax
from jax.experimental import pallas as pl
from jax.experimental.pallas import tpu as pltpu
from jax.sharding import PartitionSpec as P

EPS_LN = 1e-5
F32 = jnp.float32
BF16 = jnp.bfloat16
STREAMS = 2
RING = 12
CB = 8
CW = 512
MESH = pl.DeviceIdType.MESH
LANES = 128


def wide(tiles):
    return jnp.concatenate(tiles, axis=1)


def fused(dims, hid_hbm, len_hbm, k_hbm, v_hbm, g1_hbm, c1_hbm, wq_hbm, bq_hbm, wk_hbm, bk_hbm, wv_hbm, bv_hbm,
          wo_hbm, bo_hbm, g2_hbm, c2_hbm, f1_hbm, bf1_hbm, f2_hbm, bf2_hbm,
          out_ref, kt_ref, vt_ref,
          kbuf, vbuf, wqkv, wo, wf1, wf2,
          len_ref, g1_ref, c1_ref, bq_ref, bk_ref, bv_ref, bo_ref, g2_ref, c2_ref, bf1_ref, bf2_ref,
          state, ynorm, st_send, st_recv,
          qd_send, qd_recv, kd_send, kd_recv, q_mine, qx_send, qx_recv, kx_send, kx_recv,
          qblk, snew, sbuf, pbuf, pnew, tmix, att, kfull, vfull,
          ysend, yrecv, acc,
          fd_send, fd_recv, f_mine, fx_send, fx_recv, u_buf,
          in_sem, kv_sem, w_sem, st_ssem, st_rsem, qd_ssem, qd_rsem, qx_ssem, qx_rsem,
          at_ssem, at_rsem, y_ssem, y_rsem, fd_ssem, fd_rsem, fx_ssem, fx_rsem, u_ssem, u_rsem):
    layers, batch, dm, hw, heads, s_max, ff = dims
    hd = hw // heads
    d_total = dm * 4
    rows = batch // STREAMS
    nchunk = rows // CB
    total_chunks = layers * STREAMS * nchunk
    ff_half = ff // 2
    nt = dm // LANES
    ct = CW // LANES
    nj = ff_half // CW

    r = lax.axis_index("row")
    c = lax.axis_index("col")
    core = lax.rem(r, 2)
    chip = r // 2
    partner = r + 1 - 2 * core
    xpeer = lax.rem(r + 2, 4)
    diag = lax.rem(partner + 2, 4)
    dev_p = {"row": partner}
    dev_x = {"row": xpeer}
    dev_d = {"row": diag}
    dev_y = {"col": 1 - c}

    def rcopy(src, dst, ssem, rsem, dev):
        return pltpu.make_async_remote_copy(src_ref=src, dst_ref=dst, send_sem=ssem, recv_sem=rsem,
                                            device_id=dev, device_id_type=MESH)

    def kv_copies(ci, i):
        layer = ci // (STREAMS * nchunk)
        first = lax.rem(ci, STREAMS * nchunk) * CB
        slot = lax.rem(ci, RING)
        src, dst = ((k_hbm, kbuf), (v_hbm, vbuf))[i]
        return [pltpu.make_async_copy(src.at[layer, pl.ds(first, CB)], dst.at[slot], kv_sem.at[i, slot])]

    def kv_start(ci, i):
        for cp in kv_copies(ci, i):
            cp.start()

    def kv_wait(ci, i):
        for cp in kv_copies(ci, i):
            cp.wait()

    def w_copies(name, layer):
        if name == "qkv":
            return [pltpu.make_async_copy(w.at[layer, :, pl.ds(t * 2 * hw, 2 * hw)],
                                          wqkv.at[t, :, pl.ds(i * 2 * hw, 2 * hw)], w_sem.at[3 + t * 3 + i])
                    for t in range(2) for i, w in enumerate((wq_hbm, wk_hbm, wv_hbm))]
        src, dst, i = {"o": (wo_hbm, wo, 0), "f1": (f1_hbm, wf1, 1), "f2": (f2_hbm, wf2, 2)}[name]
        return [pltpu.make_async_copy(src.at[layer], dst, w_sem.at[i])]

    def w_start(name, layer):
        if layer < layers:
            for cp in w_copies(name, layer):
                cp.start()

    def w_wait(name, layer):
        for cp in w_copies(name, layer):
            cp.wait()

    small = [pltpu.make_async_copy(a, b, in_sem.at[n]) for n, (a, b) in enumerate((
        (hid_hbm, state), (len_hbm, len_ref), (g1_hbm, g1_ref), (c1_hbm, c1_ref), (bq_hbm, bq_ref), (bk_hbm, bk_ref),
        (bv_hbm, bv_ref), (bo_hbm, bo_ref), (g2_hbm, g2_ref), (c2_hbm, c2_ref), (bf1_hbm, bf1_ref), (bf2_hbm, bf2_ref)))]
    small[0].start()
    barrier = pltpu.get_barrier_semaphore()
    for dev in (dev_p, dev_x, dev_d, dev_y):
        pl.semaphore_signal(barrier, inc=1, device_id=dev, device_id_type=MESH)
    for cp in small[1:]:
        cp.start()
    w_start("qkv", 0)

    def prime(ci, carry):
        kv_start(ci, 0)
        kv_start(ci, 1)
        return carry

    def rsl(s):
        return pl.ds(s * rows, rows)

    def stat_copies(s, which):
        return [rcopy(st_send.at[which, s], st_recv.at[which, s, i], st_ssem.at[which, s, i], st_rsem.at[which, s, i], dev)
                for i, dev in enumerate((dev_p, dev_x, dev_d))]

    def stats_send(s, which, xv):
        p1 = xv[:, 0:128]
        p2 = p1 * p1
        for i in range(1, dm // 128):
            t = xv[:, i * 128:(i + 1) * 128]
            p1 = p1 + t
            p2 = p2 + t * t
        both = jnp.concatenate([p1, p2], axis=0)
        row = jnp.sum(both.T, axis=0, keepdims=True)
        st_send[which, s] = jnp.broadcast_to(row, (8, 2 * rows))
        for cp in stat_copies(s, which):
            cp.start()

    def norm(s, which, gain, shift):
        for cp in stat_copies(s, which):
            cp.wait()
        row = ((st_send[which, s, 0:1, :] + st_recv[which, s, 0, 0:1, :])
               + (st_recv[which, s, 1, 0:1, :] + st_recv[which, s, 2, 0:1, :]))
        n2 = 2 * rows
        eye = lax.broadcasted_iota(jnp.int32, (n2, n2), 0) == lax.broadcasted_iota(jnp.int32, (n2, n2), 1)
        col = jnp.sum(jnp.where(eye, jnp.broadcast_to(row, (n2, n2)), 0.0), axis=1, keepdims=True)
        mean = col[0:rows] * (1.0 / d_total)
        var = col[rows:] * (1.0 / d_total) - mean * mean
        rstd = lax.rsqrt(var + EPS_LN)
        xv = state[rsl(s), :].astype(F32)
        y = ((xv - mean) * rstd * gain.astype(F32) + shift.astype(F32)).astype(BF16)
        for t in range(nt):
            ynorm[t, rsl(s), :] = y[:, t * LANES:(t + 1) * LANES]

    def normed(s):
        return wide([ynorm[t, rsl(s), :] for t in range(nt)])

    def qd_copy(s, i, m):
        src, dst = ((qd_send, qd_recv), (kd_send, kd_recv))[m]
        return rcopy(src.at[s, i], dst.at[s, i], qd_ssem.at[s, i, m], qd_rsem.at[s, i, m], dev_p)

    def qx_copy(s, m):
        src, dst = ((qx_send, qx_recv), (kx_send, kx_recv))[m]
        return rcopy(src.at[s], dst.at[s], qx_ssem.at[s, m], qx_rsem.at[s, m], dev_x)

    def qkv_part(first, i, count=1):
        target = 1 - chip if i == 0 else chip
        yv = wide([ynorm[t, pl.ds(first * rows, count * rows), :] for t in range(nt)])
        every = jnp.dot(yv, wqkv[target], preferred_element_type=F32)
        for n in range(count):
            s = first + n
            res = every[n * rows:(n + 1) * rows]
            for m in range(3):
                low, high = res[:, 2 * m * hw:(2 * m + 1) * hw], res[:, (2 * m + 1) * hw:(2 * m + 2) * hw]
                q_mine[s, i, :, m * hw:(m + 1) * hw] = jnp.where(core == 0, low, high)
                away = jnp.where(core == 0, high, low).astype(BF16)
                if m == 0:
                    qd_send[s, i] = away
                    qd_copy(s, i, 0).start()
                else:
                    kd_send[s, i, :, (m - 1) * hw:m * hw] = away
            qd_copy(s, i, 1).start()

    def qkv_forward(s):
        qd_copy(s, 0, 0).wait()
        qx_send[s] = (q_mine[s, 0, :, 0:hw] + qd_recv[s, 0].astype(F32)).astype(BF16)
        qx_copy(s, 0).start()
        qd_copy(s, 0, 1).wait()
        kx_send[s] = (q_mine[s, 0, :, hw:3 * hw] + kd_recv[s, 0].astype(F32)).astype(BF16)
        qx_copy(s, 1).start()

    def own_bias(b_ref, layer):
        b = b_ref[layer:layer + 1, :].astype(F32)
        parts = [b[:, i * hw:(i + 1) * hw] for i in range(4)]
        return jnp.where(r == 0, parts[0], jnp.where(r == 1, parts[1], jnp.where(r == 2, parts[2], parts[3])))

    def expand_mat():
        hr = heads * rows
        return (lax.broadcasted_iota(jnp.int32, (hr, rows), 0) // heads
                == lax.broadcasted_iota(jnp.int32, (hr, rows), 1)).astype(F32).astype(BF16)

    def head_mask(n):
        row = lax.rem(lax.broadcasted_iota(jnp.int32, (n, hw), 0), heads)
        lane = lax.broadcasted_iota(jnp.int32, (n, hw), 1)
        return (lane >= row * hd) & (lane < row * hd + hd)

    def q_finish(s, layer):
        qd_copy(s, 1, 0).wait()
        qx_copy(s, 0).wait()
        tot = (q_mine[s, 1, :, 0:hw] + qd_recv[s, 1].astype(F32)) + qx_recv[s].astype(F32)
        q = ((tot + own_bias(bq_ref, layer)) * (hd ** -0.5)).astype(BF16)
        qblk[...] = jnp.where(head_mask(heads * rows), jnp.dot(expand_mat(), q, preferred_element_type=F32), 0.0).astype(BF16)

    def kv_finish(s, layer):
        qd_copy(s, 1, 1).wait()
        qx_copy(s, 1).wait()
        tot = (q_mine[s, 1, :, hw:3 * hw] + kd_recv[s, 1].astype(F32)) + kx_recv[s].astype(F32)
        k = (tot[:, 0:hw] + own_bias(bk_ref, layer)).astype(BF16)
        v = (tot[:, hw:2 * hw] + own_bias(bv_ref, layer)).astype(BF16)
        kfull[rsl(s), :hw] = k.astype(F32)
        vfull[rsl(s), :hw] = v.astype(F32)
        ke = jnp.dot(expand_mat(), k, preferred_element_type=F32)
        snew[...] = jnp.broadcast_to(jnp.sum(qblk[...].astype(F32) * ke, axis=1, keepdims=True), snew.shape)

    nr = CB * heads
    per = 128 // nr
    upper = lax.broadcasted_iota(jnp.int32, (8, 1), 0) < heads

    pos = lax.broadcasted_iota(jnp.int32, (nr, s_max), 1)

    def at_row(g):
        return pl.multiple_of(g * nr, nr)

    def scores_of(base, g):
        slot = lax.rem(base + g, RING)
        out = []
        for t in range(nr // 16):
            lhs = qblk[pl.ds(pl.multiple_of(at_row(g) + t * 16, 16), 16), :]
            d = [jnp.dot(lhs, kbuf[slot, t * 4 + i], preferred_element_type=F32)
                 for i in range(4)]
            out.append(jnp.where(upper, d[0][0:8], d[1][0:8]))
            out.append(jnp.where(upper, d[2][8:16], d[3][8:16]))
        return jnp.concatenate(out, axis=0)

    def softmax_of(s, g, sc):
        lens = []
        for i in range(0, CB, 2):
            b = s * rows + g * CB + i
            lens.append(jnp.where(upper, len_ref[b], len_ref[b + 1]))
        sc = jnp.where(pos < jnp.concatenate(lens, axis=0), sc, -jnp.inf)
        sn = snew[pl.ds(at_row(g), nr), 0:1]
        peak = jnp.maximum(jnp.max(sc, axis=1, keepdims=True), sn)
        e = jnp.exp(sc - peak)
        en = jnp.exp(sn - peak)
        inv = 1.0 / (jnp.sum(e, axis=1, keepdims=True) + en)
        return (e * inv).astype(BF16), jnp.broadcast_to(en * inv, (nr, LANES))

    def keep_probs(g, prob, fresh):
        for h in range(s_max // LANES):
            pbuf[h, pl.ds(at_row(g), nr), :] = prob[:, h * LANES:(h + 1) * LANES]
        pnew[pl.ds(at_row(g), nr), :] = fresh

    def probs_of(g):
        return wide([pbuf[h, pl.ds(pl.multiple_of(g // per * 128, 128), 128), :] for h in range(s_max // LANES)])

    def mix(base, g, rhs, new):
        slot = lax.rem(base + g, RING)
        seq = lax.broadcasted_iota(jnp.int32, (hw, 128), 1) // heads - lax.rem(g, per) * CB
        for b in range(CB):
            o = lax.dot_general(vbuf[slot, b], rhs, (((1,), (1,)), ((), ())), preferred_element_type=F32)
            new = jnp.where(seq == b, o, new)
        return new

    def refill(ci, i):
        @pl.when(ci + RING < total_chunks)
        def _():
            kv_start(ci + RING, i)

    def attention_pair(s, layer, g, tail):
        base = (layer * STREAMS + s) * nchunk
        kv_wait(base + g, 1)
        kv_wait(base + g + 1, 1)
        if not tail:
            kv_wait(base + g + 2, 0)
            kv_wait(base + g + 3, 0)
        sc = sbuf[...]
        rhs = probs_of(g)
        new = tmix[g // per]
        pa = softmax_of(s, g + 1, sc)
        if not tail:
            sc = scores_of(base, g + 2)
        new = mix(base, g, rhs, new)
        keep_probs(g + 1, *pa)
        rhs = probs_of(g + 1)
        if not tail:
            pa = softmax_of(s, g + 2, sc)
            sc = scores_of(base, g + 3)
        new = mix(base, g + 1, rhs, new)
        tmix[g // per] = new
        if not tail:
            keep_probs(g + 2, *pa)
            sbuf[...] = sc
        for k in range(2):
            refill(base + g + k, 1)
            if not tail:
                refill(base + g + 2 + k, 0)

    def open_ph(s, layer):
        base = (layer * STREAMS + s) * nchunk
        kv_wait(base, 0)
        kv_wait(base + 1, 0)
        first = scores_of(base, 0)
        second = scores_of(base, 1)
        kv_finish(s, layer)
        pa = softmax_of(s, 0, first)
        sbuf[...] = second
        keep_probs(0, *pa)
        refill(base, 0)
        refill(base + 1, 0)

    def attention(s, layer, lo, hi):

        def body(p, carry):
            attention_pair(s, layer, 2 * p, False)
            return carry

        stop = min(hi, nchunk - 2) // 2
        if stop - lo // 2 > 1:
            lax.fori_loop(lo // 2, stop, body, 0)
        elif stop > lo // 2:
            attention_pair(s, layer, lo, False)
        if hi == nchunk:
            attention_pair(s, layer, nchunk - 2, True)

    hrow = LANES // heads

    def att_copies(s, half):
        return [rcopy(att.at[s, r, half], att.at[s, r, half], at_ssem.at[s, i, half], at_rsem.at[s, i, half], dev)
                for i, dev in enumerate((dev_p, dev_x, dev_d))]

    def att_send(s, half):
        sel = (lax.broadcasted_iota(jnp.int32, (hrow, LANES), 1) // heads
               == lax.broadcasted_iota(jnp.int32, (hrow, LANES), 0)).astype(F32).astype(BF16)
        fresh = jnp.broadcast_to(pnew[half * LANES:(half + 1) * LANES, 0:1], (LANES, hw))
        pe = jnp.where(head_mask(LANES), fresh, 0.0).astype(BF16)
        first = s * rows + half * hrow
        o = jnp.dot(sel, pe, preferred_element_type=F32) * vfull[first:first + hrow, :hw]
        feat = lax.broadcasted_iota(jnp.int32, (hw, LANES), 0)
        lane = lax.rem(lax.broadcasted_iota(jnp.int32, (hw, LANES), 1), heads)
        t = jnp.where((feat >= lane * hd) & (feat < lane * hd + hd), tmix[half], 0.0)
        high = t.astype(BF16)
        low = (t - high.astype(F32)).astype(BF16)
        for part in (high, low):
            o = o + lax.dot_general(sel, part, (((1,), (1,)), ((), ())), preferred_element_type=F32)
        att[s, r, half] = o.astype(BF16)
        p, x, d = att_copies(s, half)
        x.start()
        d.start()
        p.start()

    def y_copy(s, which):
        return rcopy(ysend.at[which, s], yrecv.at[which, s], y_ssem.at[which, s], y_rsem.at[which, s], dev_y)

    def out_proj(s):
        for half in range(rows // hrow):
            for cp in att_copies(s, half):
                cp.wait()
        every = wide([jnp.concatenate([att[s, i, h] for h in range(rows // hrow)], axis=0) for i in range(4)])
        res = jnp.dot(every, wo[...], preferred_element_type=F32)
        ysend[0, s] = res.astype(BF16)
        y_copy(s, 0).start()

    def residual(s, which, bias):
        y_copy(s, which).wait()
        both = ysend[which, s].astype(F32) + yrecv[which, s].astype(F32)
        new = (state[rsl(s), :].astype(F32) + (both + bias.astype(F32))).astype(BF16)
        return new

    def fd_copy(s, j):
        return rcopy(fd_send.at[s, j], fd_recv.at[s, j], fd_ssem.at[s, j], fd_rsem.at[s, j], dev_p)

    def fx_copy(s, j):
        return rcopy(fx_send.at[s, j], fx_recv.at[s, j], fx_ssem.at[s, j], fx_rsem.at[s, j], dev_x)

    def u_copy(s, j, owner):
        return rcopy(u_buf.at[s, owner, j], u_buf.at[s, owner, j], u_ssem.at[s, j], u_rsem.at[s, j], dev_p)

    def fc1_part(s):
        yv = normed(s)

        def columns(owner, first, n):
            at = pl.multiple_of(owner * ff_half + first * LANES, LANES)
            return jnp.dot(yv, wf1[:, pl.ds(at, n * LANES)], preferred_element_type=F32)

        tiles = ff_half // LANES
        res = columns(1 - core, 0, tiles).astype(BF16)
        for j in range(nj):
            for t in range(ct):
                fd_send[s, j, t] = res[:, (j * ct + t) * LANES:(j * ct + t + 1) * LANES]
            fd_copy(s, j).start()
        res = columns(core, 0, tiles)
        for j in range(nj):
            f_mine[s, j] = res[:, j * CW:(j + 1) * CW]

    def fc1_forward(s, lo, hi):
        def body(j, carry):
            fd_copy(s, j).wait()
            for t in range(ct):
                fx_send[s, j, t] = (f_mine[s, j, :, t * LANES:(t + 1) * LANES] + fd_recv[s, j, t].astype(F32)).astype(BF16)
            fx_copy(s, j).start()
            return carry

        lax.fori_loop(lo, hi, body, 0)

    def fc2_dot(s, owner, lo, hi):
        off = pl.multiple_of(owner * ff_half + lo * CW, LANES)
        u = wide([u_buf[s, owner, j, t] for j in range(lo, hi) for t in range(ct)])
        return jnp.dot(u, wf2[pl.ds(off, (hi - lo) * CW), :], preferred_element_type=F32)

    def mlp(s, layer, lo, hi, plo, phi):
        def body(j, carry):
            fx_copy(s, j).wait()
            off = pl.multiple_of(core * ff_half + j * CW, LANES)
            bias = bf1_ref[layer:layer + 1, pl.ds(off, CW)].astype(F32)
            for t in range(ct):
                u = (fx_send[s, j, t].astype(F32) + fx_recv[s, j, t].astype(F32)) + bias[:, t * LANES:(t + 1) * LANES]
                u = u.astype(BF16)
                u_buf[s, core, j, t] = jnp.maximum(u, jnp.zeros_like(u))
            u_copy(s, j, core).start()
            return carry

        lax.fori_loop(lo, hi, body, 0)
        add = fc2_dot(s, core, lo, hi)
        if phi > plo:
            for j in range(plo, phi):
                u_copy(s, j, 1 - core).wait_recv()
            add = add + fc2_dot(s, 1 - core, plo, phi)
        if lo > 0:
            add = acc[s] + add
        if hi < nj:
            acc[s] = add
        else:
            ysend[1, s] = add.astype(BF16)
            y_copy(s, 1).start()
            for j in range(nj):
                u_copy(s, j, core).wait_send()

    def kv_out(layer):
        kt_ref[layer] = kfull[...].T[:hw, :].astype(BF16)
        vt_ref[layer] = vfull[...].T[:hw, :].astype(BF16)

    def gain_ph(s, which, layer):
        g, b = (g1_ref, c1_ref) if which == 0 else (g2_ref, c2_ref)
        norm(s, which, g[layer:layer + 1, :], b[layer:layer + 1, :])

    def mid_ph(s, layer):
        new = residual(s, 0, bo_ref[layer:layer + 1, :])
        state[rsl(s), :] = new
        stats_send(s, 1, new.astype(F32))

    def end_ph(s, layer):
        new = residual(s, 1, bf2_ref[layer:layer + 1, :])
        if layer == layers - 1:
            out_ref[rsl(s), :] = new
        else:
            state[rsl(s), :] = new
            stats_send(s, 0, new.astype(F32))

    small[0].wait()
    pl.semaphore_wait(barrier, 4)
    stats_send(0, 0, state[rsl(0), :].astype(F32))
    stats_send(1, 0, state[rsl(1), :].astype(F32))
    lax.fori_loop(0, RING, prime, 0)
    kfull[...] = jnp.zeros_like(kfull)
    vfull[...] = jnp.zeros_like(vfull)
    pbuf[...] = jnp.zeros_like(pbuf)
    tmix[...] = jnp.zeros_like(tmix)
    for cp in small[1:]:
        cp.wait()
    w_wait("qkv", 0)
    gain_ph(0, 0, 0)
    gain_ph(1, 0, 0)
    qkv_part(0, 0, 2)
    qkv_part(0, 1, 2)
    qkv_forward(0)
    qkv_forward(1)
    w_start("qkv", 1)
    w_start("o", 0)
    w_start("f1", 0)
    w_start("f2", 0)
    q_finish(0, 0)
    open_ph(0, 0)
    attention(0, 0, 0, nchunk // 2)
    att_send(0, 0)
    attention(0, 0, nchunk // 2, nchunk)
    att_send(0, 1)
    q4 = nchunk // 4
    for layer in range(layers):
        last = layer == layers - 1
        w_wait("o", layer)
        if last:
            out_proj(0)
        q_finish(1, layer)
        if last:
            open_ph(1, layer)
            attention(1, layer, 0, q4)
        else:
            open_ph(1, layer)
            attention(1, layer, 0, q4)
            out_proj(0)
        attention(1, layer, q4, 2 * q4)
        att_send(1, 0)
        if last:
            mid_ph(0, layer)
        attention(1, layer, 2 * q4, 3 * q4)
        if not last:
            mid_ph(0, layer)
        attention(1, layer, 3 * q4, nchunk)
        att_send(1, 1)
        w_wait("f1", layer)
        gain_ph(0, 1, layer)
        fc1_part(0)
        fc1_forward(0, 0, 3)
        out_proj(1)
        w_start("o", layer + 1)
        kv_out(layer)
        w_wait("f2", layer)
        mlp(0, layer, 0, 1, 0, 0)
        mid_ph(1, layer)
        fc1_forward(0, 3, nj)
        mlp(0, layer, 1, 2, 0, 1)
        mlp(0, layer, 2, 3, 1, 2)
        gain_ph(1, 1, layer)
        fc1_part(1)
        w_start("f1", layer + 1)
        fc1_forward(1, 0, nj if last else 4)
        mlp(0, layer, 3, nj, 2, nj)
        mlp(1, layer, 0, 1, 0, 0)
        end_ph(0, layer)
        if not last:
            fc1_forward(1, 4, nj)
        mlp(1, layer, 1, 2, 0, 1)
        if not last:
            w_wait("qkv", layer + 1)
            gain_ph(0, 0, layer + 1)
            qkv_part(0, 0)
            mlp(1, layer, 2, 3, 1, 2)
            qkv_forward(0)
            qkv_part(0, 1)
        else:
            mlp(1, layer, 2, 3, 1, 2)
        mlp(1, layer, 3, nj - 1, 2, 3)
        mlp(1, layer, nj - 1, nj, 3, nj)
        w_start("f2", layer + 1)
        if not last:
            q_finish(0, layer + 1)
            open_ph(0, layer + 1)
            attention(0, layer + 1, 0, q4)
            end_ph(1, layer)
            attention(0, layer + 1, q4, 2 * q4)
            att_send(0, 0)
            attention(0, layer + 1, 2 * q4, 3 * q4)
            gain_ph(1, 0, layer + 1)
            qkv_part(1, 0)
            attention(0, layer + 1, 3 * q4, nchunk)
            att_send(0, 1)
            qkv_forward(1)
            qkv_part(1, 1)
            w_start("qkv", layer + 2)
        else:
            end_ph(1, layer)


def finish(a_ref, b_ref, c_ref, x_ref, y_ref, z_ref):
    x_ref[...] = a_ref[...]
    y_ref[...] = b_ref[...]
    z_ref[...] = c_ref[...]


def solution(mesh):
    act_spec = P("dp", "row")
    cache_spec = P(None, "dp", ("col", "row"), None, None)
    fresh_spec = P(None, "dp", ("col", "row"), None)
    in_weight = P(None, "row", "col")
    out_weight = P(None, "col", "row")
    col_vec = P(None, "col")
    row_vec = P(None, "row")
    in_specs = (act_spec, P("dp"), cache_spec, cache_spec, row_vec, row_vec,
                in_weight, col_vec, in_weight, col_vec, in_weight, col_vec,
                out_weight, row_vec, row_vec, row_vec, in_weight, col_vec, out_weight, row_vec)

    def local_step(hidden, cache_len, k_cache, v_cache, ln1_g, ln1_b, w_q, b_q, w_k, b_k, w_v, b_v,
                   w_o, b_o, ln2_g, ln2_b, w_fc1, b_fc1, w_fc2, b_fc2):
        layers, batch, heads, s_max, hd = k_cache.shape
        dm = hidden.shape[1]
        hw = heads * hd
        ff = w_fc1.shape[2]
        rows = batch // STREAMS
        nj = ff // 2 // CW
        nt = dm // LANES
        ct = CW // LANES
        kt = k_cache.transpose(0, 1, 2, 4, 3).reshape(layers, batch, hw, s_max)
        vt = v_cache.transpose(0, 1, 2, 4, 3).reshape(layers, batch, hw, s_max)
        vm = pl.BlockSpec(memory_space=pltpu.VMEM)
        hb = pl.BlockSpec(memory_space=pl.ANY)
        hr = heads * rows
        V = pltpu.VMEM
        D = pltpu.SemaphoreType.DMA
        scratch = [
            V((RING, CB, hw, s_max), BF16), V((RING, CB, hw, s_max), BF16),
            V((2, dm, 6 * hw), BF16), V(w_o.shape[1:], BF16), V(w_fc1.shape[1:], BF16), V(w_fc2.shape[1:], BF16),
            pltpu.SMEM((batch,), jnp.int32), V((layers, dm), BF16), V((layers, dm), BF16),
            V(b_q.shape, BF16), V(b_k.shape, BF16), V(b_v.shape, BF16), V(b_o.shape, BF16),
            V((layers, dm), BF16), V((layers, dm), BF16), V(b_fc1.shape, BF16), V(b_fc2.shape, BF16),
            V((batch, dm), BF16), V((nt, batch, LANES), BF16),
            V((2, STREAMS, 8, 2 * rows), F32), V((2, STREAMS, 3, 8, 2 * rows), F32),
            V((STREAMS, 2, rows, hw), BF16), V((STREAMS, 2, rows, hw), BF16), V((STREAMS, 2, rows, 2 * hw), BF16), V((STREAMS, 2, rows, 2 * hw), BF16),
            V((STREAMS, 2, rows, 3 * hw), F32),
            V((STREAMS, rows, hw), BF16), V((STREAMS, rows, hw), BF16), V((STREAMS, rows, 2 * hw), BF16), V((STREAMS, rows, 2 * hw), BF16),
            V((hr, hw), BF16), V((hr, 128), F32), V((CB * heads, s_max), F32), V((s_max // LANES, hr, LANES), BF16), V((hr, 128), F32),
            V((hr // 128, hw, 128), F32),
            V((STREAMS, 4, hr // LANES, LANES // heads, hw), BF16), V((batch, 384), F32), V((batch, 384), F32),
            V((2, STREAMS, rows, dm), BF16), V((2, STREAMS, rows, dm), BF16), V((STREAMS, rows, dm), F32),
            V((STREAMS, nj, ct, rows, LANES), BF16), V((STREAMS, nj, ct, rows, LANES), BF16), V((STREAMS, nj, rows, CW), F32),
            V((STREAMS, nj, ct, rows, LANES), BF16), V((STREAMS, nj, ct, rows, LANES), BF16),
            V((STREAMS, 2, nj, ct, rows, LANES), BF16),
            D((12,)), D((2, RING)), D((9,)), D((2, STREAMS, 3)), D((2, STREAMS, 3)),
            D((STREAMS, 2, 2)), D((STREAMS, 2, 2)), D((STREAMS, 2)), D((STREAMS, 2)),
            D((STREAMS, 3, hr // LANES)), D((STREAMS, 3, hr // LANES)), D((2, STREAMS)), D((2, STREAMS)),
            D((STREAMS, nj)), D((STREAMS, nj)), D((STREAMS, nj)), D((STREAMS, nj)), D((STREAMS, nj)), D((STREAMS, nj)),
        ]
        out, kn, vn = pl.pallas_call(
            functools.partial(fused, (layers, batch, dm, hw, heads, s_max, ff)),
            out_shape=(jax.ShapeDtypeStruct((batch, dm), BF16),
                       jax.ShapeDtypeStruct((layers, hw, batch), BF16),
                       jax.ShapeDtypeStruct((layers, hw, batch), BF16)),
            in_specs=[hb] * 20,
            out_specs=(vm, vm, vm),
            scratch_shapes=scratch,
            compiler_params=pltpu.CompilerParams(collective_id=0, has_side_effects=True,
                                                 vmem_limit_bytes=67043328),
        )(hidden, cache_len, kt, vt, ln1_g, ln1_b, w_q, b_q, w_k, b_k, w_v, b_v,
          w_o, b_o, ln2_g, ln2_b, w_fc1, b_fc1, w_fc2, b_fc2)
        out, kn, vn = pl.pallas_call(
            finish, out_shape=tuple(jax.ShapeDtypeStruct(a.shape, a.dtype) for a in (out, kn, vn)),
            in_specs=[vm] * 3, out_specs=(vm,) * 3)(out, kn, vn)
        kn = kn.reshape(layers, heads, hd, batch).transpose(0, 3, 1, 2)
        vn = vn.reshape(layers, heads, hd, batch).transpose(0, 3, 1, 2)
        return out, kn, vn

    return jax.shard_map(local_step, mesh=mesh, in_specs=in_specs,
                         out_specs=(act_spec, fresh_spec, fresh_spec), check_vma=False)
```

```python
import functools

import jax
import jax.numpy as jnp
from jax import lax
from jax.experimental import pallas as pl
from jax.experimental.pallas import tpu as pltpu
from jax.sharding import PartitionSpec as P

EPS_LN = 1e-5
F32 = jnp.float32
BF16 = jnp.bfloat16
STREAMS = 2
RING = 10
CB = 8
CW = 512
MESH = pl.DeviceIdType.MESH
LANES = 128


def wide(tiles):
    return jnp.concatenate(tiles, axis=1)


def fused(dims, hid_hbm, len_hbm, k_hbm, v_hbm, g1_hbm, c1_hbm, wq_hbm, bq_hbm, wk_hbm, bk_hbm, wv_hbm, bv_hbm,
          wo_hbm, bo_hbm, g2_hbm, c2_hbm, f1_hbm, bf1_hbm, f2_hbm, bf2_hbm,
          out_ref, kt_ref, vt_ref,
          kbuf, vbuf, wqkv, wo, wf1, wf2,
          len_ref, g1_ref, c1_ref, bq_ref, bk_ref, bv_ref, bo_ref, g2_ref, c2_ref, bf1_ref, bf2_ref,
          state, ynorm, st_send, st_recv,
          qd_send, qd_recv, kd_send, kd_recv, q_mine, qx_send, qx_recv, kx_send, kx_recv,
          qblk, snew, sbuf, pbuf, pnew, tmix, att, kfull, vfull,
          ysend, yrecv, acc,
          fd_send, fd_recv, f_mine, fx_send, fx_recv, u_buf,
          in_sem, kv_sem, w_sem, st_ssem, st_rsem, qd_ssem, qd_rsem, qx_ssem, qx_rsem,
          at_ssem, at_rsem, y_ssem, y_rsem, fd_ssem, fd_rsem, fx_ssem, fx_rsem, u_ssem, u_rsem):
    layers, batch, dm, hw, heads, s_max, ff = dims
    hd = hw // heads
    d_total = dm * 4
    rows = batch // STREAMS
    nchunk = rows // CB
    total_chunks = layers * STREAMS * nchunk
    ff_half = ff // 2
    nt = dm // LANES
    ct = CW // LANES
    nj = ff_half // CW

    r = lax.axis_index("row")
    c = lax.axis_index("col")
    core = lax.rem(r, 2)
    chip = r // 2
    partner = r + 1 - 2 * core
    xpeer = lax.rem(r + 2, 4)
    diag = lax.rem(partner + 2, 4)
    dev_p = {"row": partner}
    dev_x = {"row": xpeer}
    dev_d = {"row": diag}
    dev_y = {"col": 1 - c}

    def rcopy(src, dst, ssem, rsem, dev):
        return pltpu.make_async_remote_copy(src_ref=src, dst_ref=dst, send_sem=ssem, recv_sem=rsem,
                                            device_id=dev, device_id_type=MESH)

    def kv_copies(ci, i):
        layer = ci // (STREAMS * nchunk)
        first = lax.rem(ci, STREAMS * nchunk) * CB
        slot = lax.rem(ci, RING)
        src, dst = ((k_hbm, kbuf), (v_hbm, vbuf))[i]
        return [pltpu.make_async_copy(src.at[layer, pl.ds(first, CB)], dst.at[slot], kv_sem.at[i, slot])]

    def kv_start(ci, i):
        for cp in kv_copies(ci, i):
            cp.start()

    def kv_wait(ci, i):
        for cp in kv_copies(ci, i):
            cp.wait()

    def w_copies(name, layer):
        if name == "qkv":
            return [pltpu.make_async_copy(w.at[layer, :, pl.ds(t * 2 * hw, 2 * hw)],
                                          wqkv.at[t, :, pl.ds(i * 2 * hw, 2 * hw)], w_sem.at[3 + t * 3 + i])
                    for t in range(2) for i, w in enumerate((wq_hbm, wk_hbm, wv_hbm))]
        src, dst, i = {"o": (wo_hbm, wo, 0), "f1": (f1_hbm, wf1, 1), "f2": (f2_hbm, wf2, 2)}[name]
        return [pltpu.make_async_copy(src.at[layer], dst, w_sem.at[i])]

    def w_start(name, layer):
        if layer < layers:
            for cp in w_copies(name, layer):
                cp.start()

    def w_wait(name, layer):
        for cp in w_copies(name, layer):
            cp.wait()

    small = [pltpu.make_async_copy(a, b, in_sem.at[n]) for n, (a, b) in enumerate((
        (hid_hbm, state), (len_hbm, len_ref), (g1_hbm, g1_ref), (c1_hbm, c1_ref), (bq_hbm, bq_ref), (bk_hbm, bk_ref),
        (bv_hbm, bv_ref), (bo_hbm, bo_ref), (g2_hbm, g2_ref), (c2_hbm, c2_ref), (bf1_hbm, bf1_ref), (bf2_hbm, bf2_ref)))]
    small[0].start()
    barrier = pltpu.get_barrier_semaphore()
    for dev in (dev_p, dev_x, dev_d, dev_y):
        pl.semaphore_signal(barrier, inc=1, device_id=dev, device_id_type=MESH)
    for cp in small[1:]:
        cp.start()
    w_start("qkv", 0)

    def prime(ci, carry):
        kv_start(ci, 0)
        kv_start(ci, 1)
        return carry

    def rsl(s):
        return pl.ds(s * rows, rows)

    def stat_copies(s, which):
        return [rcopy(st_send.at[which, s], st_recv.at[which, s, i], st_ssem.at[which, s, i], st_rsem.at[which, s, i], dev)
                for i, dev in enumerate((dev_p, dev_x, dev_d))]

    def stats_send(s, which, xv):
        p1 = xv[:, 0:128]
        p2 = p1 * p1
        for i in range(1, dm // 128):
            t = xv[:, i * 128:(i + 1) * 128]
            p1 = p1 + t
            p2 = p2 + t * t
        both = jnp.concatenate([p1, p2], axis=0)
        row = jnp.sum(both.T, axis=0, keepdims=True)
        st_send[which, s] = jnp.broadcast_to(row, (8, 2 * rows))
        for cp in stat_copies(s, which):
            cp.start()

    def norm(s, which, gain, shift):
        for cp in stat_copies(s, which):
            cp.wait()
        row = ((st_send[which, s, 0:1, :] + st_recv[which, s, 0, 0:1, :])
               + (st_recv[which, s, 1, 0:1, :] + st_recv[which, s, 2, 0:1, :]))
        n2 = 2 * rows
        eye = lax.broadcasted_iota(jnp.int32, (n2, n2), 0) == lax.broadcasted_iota(jnp.int32, (n2, n2), 1)
        col = jnp.sum(jnp.where(eye, jnp.broadcast_to(row, (n2, n2)), 0.0), axis=1, keepdims=True)
        mean = col[0:rows] * (1.0 / d_total)
        var = col[rows:] * (1.0 / d_total) - mean * mean
        rstd = lax.rsqrt(var + EPS_LN)
        xv = state[rsl(s), :].astype(F32)
        y = ((xv - mean) * rstd * gain.astype(F32) + shift.astype(F32)).astype(BF16)
        for t in range(nt):
            ynorm[t, rsl(s), :] = y[:, t * LANES:(t + 1) * LANES]

    def normed(s):
        return wide([ynorm[t, rsl(s), :] for t in range(nt)])

    def qd_copy(s, i, m):
        src, dst = ((qd_send, qd_recv), (kd_send, kd_recv))[m]
        return rcopy(src.at[s, i], dst.at[s, i], qd_ssem.at[s, i, m], qd_rsem.at[s, i, m], dev_p)

    def qx_copy(s, m):
        src, dst = ((qx_send, qx_recv), (kx_send, kx_recv))[m]
        return rcopy(src.at[s], dst.at[s], qx_ssem.at[s, m], qx_rsem.at[s, m], dev_x)

    def qkv_part(first, i, count=1):
        target = 1 - chip if i == 0 else chip
        yv = wide([ynorm[t, pl.ds(first * rows, count * rows), :] for t in range(nt)])
        every = jnp.dot(yv, wqkv[target], preferred_element_type=F32)
        for n in range(count):
            s = first + n
            res = every[n * rows:(n + 1) * rows]
            for m in range(3):
                low, high = res[:, 2 * m * hw:(2 * m + 1) * hw], res[:, (2 * m + 1) * hw:(2 * m + 2) * hw]
                q_mine[s, i, :, m * hw:(m + 1) * hw] = jnp.where(core == 0, low, high)
                away = jnp.where(core == 0, high, low).astype(BF16)
                if m == 0:
                    qd_send[s, i] = away
                    qd_copy(s, i, 0).start()
                else:
                    kd_send[s, i, :, (m - 1) * hw:m * hw] = away
            qd_copy(s, i, 1).start()

    def qkv_forward(s):
        qd_copy(s, 0, 0).wait()
        qx_send[s] = (q_mine[s, 0, :, 0:hw] + qd_recv[s, 0].astype(F32)).astype(BF16)
        qx_copy(s, 0).start()
        qd_copy(s, 0, 1).wait()
        kx_send[s] = (q_mine[s, 0, :, hw:3 * hw] + kd_recv[s, 0].astype(F32)).astype(BF16)
        qx_copy(s, 1).start()

    def own_bias(b_ref, layer):
        b = b_ref[layer:layer + 1, :].astype(F32)
        parts = [b[:, i * hw:(i + 1) * hw] for i in range(4)]
        return jnp.where(r == 0, parts[0], jnp.where(r == 1, parts[1], jnp.where(r == 2, parts[2], parts[3])))

    def expand_mat():
        hr = heads * rows
        return (lax.broadcasted_iota(jnp.int32, (hr, rows), 0) // heads
                == lax.broadcasted_iota(jnp.int32, (hr, rows), 1)).astype(F32).astype(BF16)

    def head_mask(n):
        row = lax.rem(lax.broadcasted_iota(jnp.int32, (n, hw), 0), heads)
        lane = lax.broadcasted_iota(jnp.int32, (n, hw), 1)
        return (lane >= row * hd) & (lane < row * hd + hd)

    def q_finish(s, layer):
        qd_copy(s, 1, 0).wait()
        qx_copy(s, 0).wait()
        tot = (q_mine[s, 1, :, 0:hw] + qd_recv[s, 1].astype(F32)) + qx_recv[s].astype(F32)
        q = ((tot + own_bias(bq_ref, layer)) * (hd ** -0.5)).astype(BF16)
        qblk[...] = jnp.where(head_mask(heads * rows), jnp.dot(expand_mat(), q, preferred_element_type=F32), 0.0).astype(BF16)

    def kv_finish(s, layer):
        qd_copy(s, 1, 1).wait()
        qx_copy(s, 1).wait()
        tot = (q_mine[s, 1, :, hw:3 * hw] + kd_recv[s, 1].astype(F32)) + kx_recv[s].astype(F32)
        k = (tot[:, 0:hw] + own_bias(bk_ref, layer)).astype(BF16)
        v = (tot[:, hw:2 * hw] + own_bias(bv_ref, layer)).astype(BF16)
        kfull[rsl(s), :hw] = k.astype(F32)
        vfull[rsl(s), :hw] = v.astype(F32)
        ke = jnp.dot(expand_mat(), k, preferred_element_type=F32)
        snew[...] = jnp.broadcast_to(jnp.sum(qblk[...].astype(F32) * ke, axis=1, keepdims=True), snew.shape)

    nr = CB * heads
    per = 128 // nr
    upper = lax.broadcasted_iota(jnp.int32, (8, 1), 0) < heads

    pos = lax.broadcasted_iota(jnp.int32, (nr, s_max), 1)

    def at_row(g):
        return pl.multiple_of(g * nr, nr)

    def scores_of(base, g):
        slot = lax.rem(base + g, RING)
        out = []
        for t in range(nr // 16):
            lhs = qblk[pl.ds(pl.multiple_of(at_row(g) + t * 16, 16), 16), :]
            d = [jnp.dot(lhs, kbuf[slot, t * 4 + i], preferred_element_type=F32)
                 for i in range(4)]
            out.append(jnp.where(upper, d[0][0:8], d[1][0:8]))
            out.append(jnp.where(upper, d[2][8:16], d[3][8:16]))
        return jnp.concatenate(out, axis=0)

    def softmax_of(s, g, sc):
        lens = []
        for i in range(0, CB, 2):
            b = s * rows + g * CB + i
            lens.append(jnp.where(upper, len_ref[b], len_ref[b + 1]))
        sc = jnp.where(pos < jnp.concatenate(lens, axis=0), sc, -jnp.inf)
        sn = snew[pl.ds(at_row(g), nr), 0:1]
        peak = jnp.maximum(jnp.max(sc, axis=1, keepdims=True), sn)
        e = jnp.exp(sc - peak)
        en = jnp.exp(sn - peak)
        inv = 1.0 / (jnp.sum(e, axis=1, keepdims=True) + en)
        return (e * inv).astype(BF16), jnp.broadcast_to(en * inv, (nr, LANES))

    def keep_probs(g, prob, fresh):
        for h in range(s_max // LANES):
            pbuf[h, pl.ds(at_row(g), nr), :] = prob[:, h * LANES:(h + 1) * LANES]
        pnew[pl.ds(at_row(g), nr), :] = fresh

    def probs_of(g):
        return wide([pbuf[h, pl.ds(pl.multiple_of(g // per * 128, 128), 128), :] for h in range(s_max // LANES)])

    def mix(base, g, rhs, new):
        slot = lax.rem(base + g, RING)
        seq = lax.broadcasted_iota(jnp.int32, (hw, 128), 1) // heads - lax.rem(g, per) * CB
        for b in range(CB):
            o = lax.dot_general(vbuf[slot, b], rhs, (((1,), (1,)), ((), ())), preferred_element_type=F32)
            new = jnp.where(seq == b, o, new)
        return new

    def refill(ci, i):
        @pl.when(ci + RING < total_chunks)
        def _():
            kv_start(ci + RING, i)

    def attention_pair(s, layer, g, tail):
        base = (layer * STREAMS + s) * nchunk
        kv_wait(base + g, 1)
        kv_wait(base + g + 1, 1)
        if not tail:
            kv_wait(base + g + 2, 0)
            kv_wait(base + g + 3, 0)
        sc = sbuf[...]
        rhs = probs_of(g)
        new = tmix[g // per]
        pa = softmax_of(s, g + 1, sc)
        if not tail:
            sc = scores_of(base, g + 2)
        new = mix(base, g, rhs, new)
        keep_probs(g + 1, *pa)
        rhs = probs_of(g + 1)
        if not tail:
            pa = softmax_of(s, g + 2, sc)
            sc = scores_of(base, g + 3)
        new = mix(base, g + 1, rhs, new)
        tmix[g // per] = new
        if not tail:
            keep_probs(g + 2, *pa)
            sbuf[...] = sc
        for k in range(2):
            refill(base + g + k, 1)
            if not tail:
                refill(base + g + 2 + k, 0)

    def open_ph(s, layer):
        base = (layer * STREAMS + s) * nchunk
        kv_wait(base, 0)
        kv_wait(base + 1, 0)
        first = scores_of(base, 0)
        second = scores_of(base, 1)
        kv_finish(s, layer)
        pa = softmax_of(s, 0, first)
        sbuf[...] = second
        keep_probs(0, *pa)
        refill(base, 0)
        refill(base + 1, 0)

    def attention(s, layer, lo, hi):

        def body(p, carry):
            attention_pair(s, layer, 2 * p, False)
            return carry

        stop = min(hi, nchunk - 2) // 2
        if stop - lo // 2 > 1:
            lax.fori_loop(lo // 2, stop, body, 0)
        elif stop > lo // 2:
            attention_pair(s, layer, lo, False)
        if hi == nchunk:
            attention_pair(s, layer, nchunk - 2, True)

    hrow = LANES // heads

    def att_copies(s, half):
        return [rcopy(att.at[s, r, half], att.at[s, r, half], at_ssem.at[s, i, half], at_rsem.at[s, i, half], dev)
                for i, dev in enumerate((dev_p, dev_x, dev_d))]

    def att_send(s, half):
        sel = (lax.broadcasted_iota(jnp.int32, (hrow, LANES), 1) // heads
               == lax.broadcasted_iota(jnp.int32, (hrow, LANES), 0)).astype(F32).astype(BF16)
        fresh = jnp.broadcast_to(pnew[half * LANES:(half + 1) * LANES, 0:1], (LANES, hw))
        pe = jnp.where(head_mask(LANES), fresh, 0.0).astype(BF16)
        first = s * rows + half * hrow
        o = jnp.dot(sel, pe, preferred_element_type=F32) * vfull[first:first + hrow, :hw]
        feat = lax.broadcasted_iota(jnp.int32, (hw, LANES), 0)
        lane = lax.rem(lax.broadcasted_iota(jnp.int32, (hw, LANES), 1), heads)
        t = jnp.where((feat >= lane * hd) & (feat < lane * hd + hd), tmix[half], 0.0)
        high = t.astype(BF16)
        low = (t - high.astype(F32)).astype(BF16)
        for part in (high, low):
            o = o + lax.dot_general(sel, part, (((1,), (1,)), ((), ())), preferred_element_type=F32)
        att[s, r, half] = o.astype(BF16)
        p, x, d = att_copies(s, half)
        x.start()
        d.start()
        p.start()

    def y_copy(s, which):
        return rcopy(ysend.at[which, s], yrecv.at[which, s], y_ssem.at[which, s], y_rsem.at[which, s], dev_y)

    def out_proj(s):
        for half in range(rows // hrow):
            for cp in att_copies(s, half):
                cp.wait()
        every = wide([jnp.concatenate([att[s, i, h] for h in range(rows // hrow)], axis=0) for i in range(4)])
        res = jnp.dot(every, wo[...], preferred_element_type=F32)
        ysend[0, s] = res.astype(BF16)
        y_copy(s, 0).start()

    def residual(s, which, bias):
        y_copy(s, which).wait()
        both = ysend[which, s].astype(F32) + yrecv[which, s].astype(F32)
        new = (state[rsl(s), :].astype(F32) + (both + bias.astype(F32))).astype(BF16)
        return new

    def fd_copy(s, j):
        return rcopy(fd_send.at[s, j], fd_recv.at[s, j], fd_ssem.at[s, j], fd_rsem.at[s, j], dev_p)

    def fx_copy(s, j):
        return rcopy(fx_send.at[s, j], fx_recv.at[s, j], fx_ssem.at[s, j], fx_rsem.at[s, j], dev_x)

    def u_copy(s, j, owner):
        return rcopy(u_buf.at[s, owner, j], u_buf.at[s, owner, j], u_ssem.at[s, j], u_rsem.at[s, j], dev_p)

    def fc1_part(s):
        yv = normed(s)

        def columns(owner, first, n):
            at = pl.multiple_of(owner * ff_half + first * LANES, LANES)
            return jnp.dot(yv, wf1[:, pl.ds(at, n * LANES)], preferred_element_type=F32)

        tiles = ff_half // LANES
        res = columns(1 - core, 0, tiles).astype(BF16)
        for j in range(nj):
            for t in range(ct):
                fd_send[s, j, t] = res[:, (j * ct + t) * LANES:(j * ct + t + 1) * LANES]
            fd_copy(s, j).start()
        res = columns(core, 0, tiles)
        for j in range(nj):
            f_mine[s, j] = res[:, j * CW:(j + 1) * CW]

    def fc1_forward(s, lo, hi):
        def body(j, carry):
            fd_copy(s, j).wait()
            for t in range(ct):
                fx_send[s, j, t] = (f_mine[s, j, :, t * LANES:(t + 1) * LANES] + fd_recv[s, j, t].astype(F32)).astype(BF16)
            fx_copy(s, j).start()
            return carry

        lax.fori_loop(lo, hi, body, 0)

    def fc2_dot(s, owner, lo, hi):
        off = pl.multiple_of(owner * ff_half + lo * CW, LANES)
        u = wide([u_buf[s, owner, j, t] for j in range(lo, hi) for t in range(ct)])
        return jnp.dot(u, wf2[pl.ds(off, (hi - lo) * CW), :], preferred_element_type=F32)

    def mlp(s, layer, lo, hi, plo, phi):
        def body(j, carry):
            fx_copy(s, j).wait()
            off = pl.multiple_of(core * ff_half + j * CW, LANES)
            bias = bf1_ref[layer:layer + 1, pl.ds(off, CW)].astype(F32)
            for t in range(ct):
                u = (fx_send[s, j, t].astype(F32) + fx_recv[s, j, t].astype(F32)) + bias[:, t * LANES:(t + 1) * LANES]
                u = u.astype(BF16)
                u_buf[s, core, j, t] = jnp.maximum(u, jnp.zeros_like(u))
            u_copy(s, j, core).start()
            return carry

        lax.fori_loop(lo, hi, body, 0)
        add = fc2_dot(s, core, lo, hi)
        if phi > plo:
            for j in range(plo, phi):
                u_copy(s, j, 1 - core).wait_recv()
            add = add + fc2_dot(s, 1 - core, plo, phi)
        if lo > 0:
            add = acc[s] + add
        if hi < nj:
            acc[s] = add
        else:
            ysend[1, s] = add.astype(BF16)
            y_copy(s, 1).start()
            for j in range(nj):
                u_copy(s, j, core).wait_send()

    def kv_out(layer):
        kt_ref[layer] = kfull[...].T[:hw, :].astype(BF16)
        vt_ref[layer] = vfull[...].T[:hw, :].astype(BF16)

    def gain_ph(s, which, layer):
        g, b = (g1_ref, c1_ref) if which == 0 else (g2_ref, c2_ref)
        norm(s, which, g[layer:layer + 1, :], b[layer:layer + 1, :])

    def mid_ph(s, layer):
        new = residual(s, 0, bo_ref[layer:layer + 1, :])
        state[rsl(s), :] = new
        stats_send(s, 1, new.astype(F32))

    def end_ph(s, layer):
        new = residual(s, 1, bf2_ref[layer:layer + 1, :])
        if layer == layers - 1:
            out_ref[rsl(s), :] = new
        else:
            state[rsl(s), :] = new
            stats_send(s, 0, new.astype(F32))

    one, two = range(STREAMS)
    small[0].wait()
    pl.semaphore_wait(barrier, 4)
    stats_send(one, 0, state[rsl(one), :].astype(F32))
    stats_send(two, 0, state[rsl(two), :].astype(F32))
    lax.fori_loop(0, RING, prime, 0)
    kfull[...] = jnp.zeros_like(kfull)
    vfull[...] = jnp.zeros_like(vfull)
    pbuf[...] = jnp.zeros_like(pbuf)
    tmix[...] = jnp.zeros_like(tmix)
    for cp in small[1:]:
        cp.wait()
    w_wait("qkv", 0)
    gain_ph(one, 0, 0)
    gain_ph(two, 0, 0)
    qkv_part(one, 0, 2)
    qkv_part(one, 1, 2)
    qkv_forward(one)
    qkv_forward(two)
    w_start("qkv", 1)
    w_start("o", 0)
    w_start("f1", 0)
    w_start("f2", 0)
    q_finish(one, 0)
    open_ph(one, 0)
    attention(one, 0, 0, nchunk // 2)
    att_send(one, 0)
    attention(one, 0, nchunk // 2, nchunk)
    att_send(one, 1)
    q4 = nchunk // 4
    for layer in range(layers):
        last = layer == layers - 1
        w_wait("o", layer)
        if last:
            out_proj(one)
        q_finish(two, layer)
        if last:
            open_ph(two, layer)
            attention(two, layer, 0, q4)
        else:
            open_ph(two, layer)
            attention(two, layer, 0, q4)
            out_proj(one)
        attention(two, layer, q4, 2 * q4)
        if last:
            mid_ph(one, layer)
        att_send(two, 0)
        attention(two, layer, 2 * q4, 3 * q4)
        if not last:
            mid_ph(one, layer)
        attention(two, layer, 3 * q4, nchunk)
        att_send(two, 1)
        w_wait("f1", layer)
        gain_ph(one, 1, layer)
        fc1_part(one)
        fc1_forward(one, 0, 3)
        out_proj(two)
        w_start("o", layer + 1)
        kv_out(layer)
        w_wait("f2", layer)
        mlp(one, layer, 0, 1, 0, 0)
        mid_ph(two, layer)
        fc1_forward(one, 3, nj)
        mlp(one, layer, 1, 2, 0, 1)
        mlp(one, layer, 2, 3, 1, 2)
        gain_ph(two, 1, layer)
        fc1_part(two)
        w_start("f1", layer + 1)
        fc1_forward(two, 0, nj if last else 4)
        mlp(one, layer, 3, nj, 2, nj)
        mlp(two, layer, 0, 1, 0, 0)
        end_ph(one, layer)
        if not last:
            fc1_forward(two, 4, nj)
        mlp(two, layer, 1, 2, 0, 1)
        if not last:
            w_wait("qkv", layer + 1)
            gain_ph(one, 0, layer + 1)
            qkv_part(one, 0)
            mlp(two, layer, 2, 3, 1, 2)
            qkv_forward(one)
            qkv_part(one, 1)
        else:
            mlp(two, layer, 2, 3, 1, 2)
        mlp(two, layer, 3, nj - 1, 2, 3)
        mlp(two, layer, nj - 1, nj, 3, nj)
        w_start("f2", layer + 1)
        if not last:
            q_finish(one, layer + 1)
            open_ph(one, layer + 1)
            attention(one, layer + 1, 0, q4)
            end_ph(two, layer)
            attention(one, layer + 1, q4, 2 * q4)
            att_send(one, 0)
            attention(one, layer + 1, 2 * q4, 3 * q4)
            gain_ph(two, 0, layer + 1)
            qkv_part(two, 0)
            attention(one, layer + 1, 3 * q4, nchunk)
            att_send(one, 1)
            qkv_forward(two)
            qkv_part(two, 1)
            w_start("qkv", layer + 2)
        else:
            end_ph(two, layer)


def finish(a_ref, b_ref, c_ref, x_ref, y_ref, z_ref, sem):
    copies = [pltpu.make_async_copy(a, b, sem.at[n])
              for n, (a, b) in enumerate(((a_ref, x_ref), (b_ref, y_ref), (c_ref, z_ref)))]
    for cp in copies:
        cp.start()
    for cp in copies:
        cp.wait()


def solution(mesh):
    act_spec = P("dp", "row")
    cache_spec = P(None, "dp", ("col", "row"), None, None)
    fresh_spec = P(None, "dp", ("col", "row"), None)
    in_weight = P(None, "row", "col")
    out_weight = P(None, "col", "row")
    col_vec = P(None, "col")
    row_vec = P(None, "row")
    in_specs = (act_spec, P("dp"), cache_spec, cache_spec, row_vec, row_vec,
                in_weight, col_vec, in_weight, col_vec, in_weight, col_vec,
                out_weight, row_vec, row_vec, row_vec, in_weight, col_vec, out_weight, row_vec)

    def local_step(hidden, cache_len, k_cache, v_cache, ln1_g, ln1_b, w_q, b_q, w_k, b_k, w_v, b_v,
                   w_o, b_o, ln2_g, ln2_b, w_fc1, b_fc1, w_fc2, b_fc2):
        layers, batch, heads, s_max, hd = k_cache.shape
        dm = hidden.shape[1]
        hw = heads * hd
        ff = w_fc1.shape[2]
        rows = batch // STREAMS
        nj = ff // 2 // CW
        nt = dm // LANES
        ct = CW // LANES
        kt = k_cache.transpose(0, 1, 2, 4, 3).reshape(layers, batch, hw, s_max)
        vt = v_cache.transpose(0, 1, 2, 4, 3).reshape(layers, batch, hw, s_max)
        vm = pl.BlockSpec(memory_space=pltpu.VMEM)
        hb = pl.BlockSpec(memory_space=pl.ANY)
        hr = heads * rows
        V = pltpu.VMEM
        D = pltpu.SemaphoreType.DMA
        scratch = [
            V((RING, CB, hw, s_max), BF16), V((RING, CB, hw, s_max), BF16),
            V((2, dm, 6 * hw), BF16), V(w_o.shape[1:], BF16), V(w_fc1.shape[1:], BF16), V(w_fc2.shape[1:], BF16),
            pltpu.SMEM((batch,), jnp.int32), V((layers, dm), BF16), V((layers, dm), BF16),
            V(b_q.shape, BF16), V(b_k.shape, BF16), V(b_v.shape, BF16), V(b_o.shape, BF16),
            V((layers, dm), BF16), V((layers, dm), BF16), V(b_fc1.shape, BF16), V(b_fc2.shape, BF16),
            V((batch, dm), BF16), V((nt, batch, LANES), BF16),
            V((2, STREAMS, 8, 2 * rows), F32), V((2, STREAMS, 3, 8, 2 * rows), F32),
            V((STREAMS, 2, rows, hw), BF16), V((STREAMS, 2, rows, hw), BF16), V((STREAMS, 2, rows, 2 * hw), BF16), V((STREAMS, 2, rows, 2 * hw), BF16),
            V((STREAMS, 2, rows, 3 * hw), F32),
            V((STREAMS, rows, hw), BF16), V((STREAMS, rows, hw), BF16), V((STREAMS, rows, 2 * hw), BF16), V((STREAMS, rows, 2 * hw), BF16),
            V((hr, hw), BF16), V((hr, 128), F32), V((CB * heads, s_max), F32), V((s_max // LANES, hr, LANES), BF16), V((hr, 128), F32),
            V((hr // 128, hw, 128), F32),
            V((STREAMS, 4, hr // LANES, LANES // heads, hw), BF16), V((batch, 384), F32), V((batch, 384), F32),
            V((2, STREAMS, rows, dm), BF16), V((2, STREAMS, rows, dm), BF16), V((STREAMS, rows, dm), F32),
            V((STREAMS, nj, ct, rows, LANES), BF16), V((STREAMS, nj, ct, rows, LANES), BF16), V((STREAMS, nj, rows, CW), F32),
            V((STREAMS, nj, ct, rows, LANES), BF16), V((STREAMS, nj, ct, rows, LANES), BF16),
            V((STREAMS, 2, nj, ct, rows, LANES), BF16),
            D((12,)), D((2, RING)), D((9,)), D((2, STREAMS, 3)), D((2, STREAMS, 3)),
            D((STREAMS, 2, 2)), D((STREAMS, 2, 2)), D((STREAMS, 2)), D((STREAMS, 2)),
            D((STREAMS, 3, hr // LANES)), D((STREAMS, 3, hr // LANES)), D((2, STREAMS)), D((2, STREAMS)),
            D((STREAMS, nj)), D((STREAMS, nj)), D((STREAMS, nj)), D((STREAMS, nj)), D((STREAMS, nj)), D((STREAMS, nj)),
        ]
        out, kn, vn = pl.pallas_call(
            functools.partial(fused, (layers, batch, dm, hw, heads, s_max, ff)),
            out_shape=(V((batch, dm), BF16), V((layers, hw, batch), BF16), V((layers, hw, batch), BF16)),
            in_specs=[hb] * 20,
            out_specs=(vm, vm, vm),
            scratch_shapes=scratch,
            compiler_params=pltpu.CompilerParams(collective_id=0, has_side_effects=True,
                                                 vmem_limit_bytes=60000000),
        )(hidden, cache_len, kt, vt, ln1_g, ln1_b, w_q, b_q, w_k, b_k, w_v, b_v,
          w_o, b_o, ln2_g, ln2_b, w_fc1, b_fc1, w_fc2, b_fc2)
        out, kn, vn = pl.pallas_call(
            finish, out_shape=tuple(jax.ShapeDtypeStruct(a.shape, a.dtype) for a in (out, kn, vn)),
            in_specs=[vm] * 3, out_specs=(hb,) * 3, scratch_shapes=[D((3,))],
            compiler_params=pltpu.CompilerParams(vmem_limit_bytes=4 << 20))(*(pltpu.with_memory_space_constraint(a, pltpu.VMEM) for a in (out, kn, vn)))
        kn = kn.reshape(layers, heads, hd, batch).transpose(0, 3, 1, 2)
        vn = vn.reshape(layers, heads, hd, batch).transpose(0, 3, 1, 2)
        return out, kn, vn

    return jax.shard_map(local_step, mesh=mesh, in_specs=in_specs,
                         out_specs=(act_spec, fresh_spec, fresh_spec), check_vma=False)
```

```python
import functools

import jax
import jax.numpy as jnp
from jax import lax
from jax.experimental import pallas as pl
from jax.experimental.pallas import tpu as pltpu
from jax.sharding import PartitionSpec as P

EPS_LN = 1e-5
F32 = jnp.float32
BF16 = jnp.bfloat16
STREAMS = 2
RING = 10
CB = 8
CW = 512
MESH = pl.DeviceIdType.MESH
LANES = 128


def wide(tiles):
    return jnp.concatenate(tiles, axis=1)


def fused(dims, hid_hbm, len_hbm, k_hbm, v_hbm, g1_hbm, c1_hbm, wq_hbm, bq_hbm, wk_hbm, bk_hbm, wv_hbm, bv_hbm,
          wo_hbm, bo_hbm, g2_hbm, c2_hbm, f1_hbm, bf1_hbm, f2_hbm, bf2_hbm,
          out_ref, kt_ref, vt_ref,
          kbuf, vbuf, wqkv, wo, wf1, wf2,
          len_ref, g1_ref, c1_ref, bq_ref, bk_ref, bv_ref, bo_ref, g2_ref, c2_ref, bf1_ref, bf2_ref,
          state, ynorm, st_send, st_recv,
          qd_send, qd_recv, kd_send, kd_recv, q_mine, qx_send, qx_recv, kx_send, kx_recv,
          qblk, snew, sbuf, pbuf, pnew, tmix, att, kfull, vfull,
          ysend, yrecv, acc,
          fd_send, fd_recv, f_mine, fx_send, fx_recv, u_buf,
          in_sem, kv_sem, w_sem, st_ssem, st_rsem, qd_ssem, qd_rsem, qx_ssem, qx_rsem,
          at_ssem, at_rsem, y_ssem, y_rsem, fd_ssem, fd_rsem, fx_ssem, fx_rsem, u_ssem, u_rsem):
    layers, batch, dm, hw, heads, s_max, ff = dims
    hd = hw // heads
    d_total = dm * 4
    rows = batch // STREAMS
    nchunk = rows // CB
    total_chunks = layers * STREAMS * nchunk
    ff_half = ff // 2
    nt = dm // LANES
    ct = CW // LANES
    nj = ff_half // CW

    r = lax.axis_index("row")
    c = lax.axis_index("col")
    core = lax.rem(r, 2)
    chip = r // 2
    partner = r + 1 - 2 * core
    xpeer = lax.rem(r + 2, 4)
    diag = lax.rem(partner + 2, 4)
    dev_p = {"row": partner}
    dev_x = {"row": xpeer}
    dev_d = {"row": diag}
    dev_y = {"col": 1 - c}

    def rcopy(src, dst, ssem, rsem, dev):
        return pltpu.make_async_remote_copy(src_ref=src, dst_ref=dst, send_sem=ssem, recv_sem=rsem,
                                            device_id=dev, device_id_type=MESH)

    def kv_copies(ci, i):
        layer = ci // (STREAMS * nchunk)
        first = lax.rem(ci, STREAMS * nchunk) * CB
        slot = lax.rem(ci, RING)
        src, dst = ((k_hbm, kbuf), (v_hbm, vbuf))[i]
        return [pltpu.make_async_copy(src.at[layer, pl.ds(first, CB)], dst.at[slot], kv_sem.at[i, slot])]

    def kv_start(ci, i):
        for cp in kv_copies(ci, i):
            cp.start()

    def kv_wait(ci, i):
        for cp in kv_copies(ci, i):
            cp.wait()

    def w_copies(name, layer):
        if name == "qkv":
            return [pltpu.make_async_copy(w.at[layer, :, pl.ds(t * 2 * hw, 2 * hw)],
                                          wqkv.at[t, :, pl.ds(i * 2 * hw, 2 * hw)], w_sem.at[3 + t * 3 + i])
                    for t in range(2) for i, w in enumerate((wq_hbm, wk_hbm, wv_hbm))]
        src, dst, i = {"o": (wo_hbm, wo, 0), "f1": (f1_hbm, wf1, 1), "f2": (f2_hbm, wf2, 2)}[name]
        return [pltpu.make_async_copy(src.at[layer], dst, w_sem.at[i])]

    def w_start(name, layer):
        if layer < layers:
            for cp in w_copies(name, layer):
                cp.start()

    def w_wait(name, layer):
        for cp in w_copies(name, layer):
            cp.wait()

    small = [pltpu.make_async_copy(a, b, in_sem.at[n]) for n, (a, b) in enumerate((
        (hid_hbm, state), (len_hbm, len_ref), (g1_hbm, g1_ref), (c1_hbm, c1_ref), (bq_hbm, bq_ref), (bk_hbm, bk_ref),
        (bv_hbm, bv_ref), (bo_hbm, bo_ref), (g2_hbm, g2_ref), (c2_hbm, c2_ref), (bf1_hbm, bf1_ref), (bf2_hbm, bf2_ref)))]
    small[0].start()
    barrier = pltpu.get_barrier_semaphore()
    for dev in (dev_p, dev_x, dev_d, dev_y):
        pl.semaphore_signal(barrier, inc=1, device_id=dev, device_id_type=MESH)
    for cp in small[1:]:
        cp.start()
    w_start("qkv", 0)

    def prime(ci, carry):
        kv_start(ci, 0)
        kv_start(ci, 1)
        return carry

    def rsl(s):
        return pl.ds(s * rows, rows)

    def stat_copies(s, which):
        return [rcopy(st_send.at[which, s], st_recv.at[which, s, i], st_ssem.at[which, s, i], st_rsem.at[which, s, i], dev)
                for i, dev in enumerate((dev_p, dev_x, dev_d))]

    def stats_send(s, which, xv):
        p1 = xv[:, 0:128]
        p2 = p1 * p1
        for i in range(1, dm // 128):
            t = xv[:, i * 128:(i + 1) * 128]
            p1 = p1 + t
            p2 = p2 + t * t
        both = jnp.concatenate([p1, p2], axis=0)
        row = jnp.sum(both.T, axis=0, keepdims=True)
        st_send[which, s] = jnp.broadcast_to(row, (8, 2 * rows))
        for cp in stat_copies(s, which):
            cp.start()

    def norm(s, which, gain, shift):
        for cp in stat_copies(s, which):
            cp.wait()
        row = ((st_send[which, s, 0:1, :] + st_recv[which, s, 0, 0:1, :])
               + (st_recv[which, s, 1, 0:1, :] + st_recv[which, s, 2, 0:1, :]))
        n2 = 2 * rows
        eye = lax.broadcasted_iota(jnp.int32, (n2, n2), 0) == lax.broadcasted_iota(jnp.int32, (n2, n2), 1)
        col = jnp.sum(jnp.where(eye, jnp.broadcast_to(row, (n2, n2)), 0.0), axis=1, keepdims=True)
        mean = col[0:rows] * (1.0 / d_total)
        var = col[rows:] * (1.0 / d_total) - mean * mean
        rstd = lax.rsqrt(var + EPS_LN)
        xv = state[rsl(s), :].astype(F32)
        y = ((xv - mean) * rstd * gain.astype(F32) + shift.astype(F32)).astype(BF16)
        for t in range(nt):
            ynorm[t, rsl(s), :] = y[:, t * LANES:(t + 1) * LANES]

    def normed(s):
        return wide([ynorm[t, rsl(s), :] for t in range(nt)])

    def qd_copy(s, i, m):
        src, dst = ((qd_send, qd_recv), (kd_send, kd_recv))[m]
        return rcopy(src.at[s, i], dst.at[s, i], qd_ssem.at[s, i, m], qd_rsem.at[s, i, m], dev_p)

    def qx_copy(s, m):
        src, dst = ((qx_send, qx_recv), (kx_send, kx_recv))[m]
        return rcopy(src.at[s], dst.at[s], qx_ssem.at[s, m], qx_rsem.at[s, m], dev_x)

    def qkv_part(first, i, count=1):
        target = 1 - chip if i == 0 else chip
        yv = wide([ynorm[t, pl.ds(first * rows, count * rows), :] for t in range(nt)])
        every = jnp.dot(yv, wqkv[target], preferred_element_type=F32)
        for n in range(count):
            s = first + n
            res = every[n * rows:(n + 1) * rows]
            for m in range(3):
                low, high = res[:, 2 * m * hw:(2 * m + 1) * hw], res[:, (2 * m + 1) * hw:(2 * m + 2) * hw]
                q_mine[s, i, :, m * hw:(m + 1) * hw] = jnp.where(core == 0, low, high)
                away = jnp.where(core == 0, high, low).astype(BF16)
                if m == 0:
                    qd_send[s, i] = away
                    qd_copy(s, i, 0).start()
                else:
                    kd_send[s, i, :, (m - 1) * hw:m * hw] = away
            qd_copy(s, i, 1).start()

    def qkv_forward(s):
        qd_copy(s, 0, 0).wait()
        qx_send[s] = (q_mine[s, 0, :, 0:hw] + qd_recv[s, 0].astype(F32)).astype(BF16)
        qx_copy(s, 0).start()
        qd_copy(s, 0, 1).wait()
        kx_send[s] = (q_mine[s, 0, :, hw:3 * hw] + kd_recv[s, 0].astype(F32)).astype(BF16)
        qx_copy(s, 1).start()

    def own_bias(b_ref, layer):
        b = b_ref[layer:layer + 1, :].astype(F32)
        parts = [b[:, i * hw:(i + 1) * hw] for i in range(4)]
        return jnp.where(r == 0, parts[0], jnp.where(r == 1, parts[1], jnp.where(r == 2, parts[2], parts[3])))

    def expand_mat():
        hr = heads * rows
        return (lax.broadcasted_iota(jnp.int32, (hr, rows), 0) // heads
                == lax.broadcasted_iota(jnp.int32, (hr, rows), 1)).astype(F32).astype(BF16)

    def head_mask(n):
        row = lax.rem(lax.broadcasted_iota(jnp.int32, (n, hw), 0), heads)
        lane = lax.broadcasted_iota(jnp.int32, (n, hw), 1)
        return (lane >= row * hd) & (lane < row * hd + hd)

    def q_finish(s, layer):
        qd_copy(s, 1, 0).wait()
        qx_copy(s, 0).wait()
        tot = (q_mine[s, 1, :, 0:hw] + qd_recv[s, 1].astype(F32)) + qx_recv[s].astype(F32)
        q = ((tot + own_bias(bq_ref, layer)) * (hd ** -0.5)).astype(BF16)
        qblk[...] = jnp.where(head_mask(heads * rows), jnp.dot(expand_mat(), q, preferred_element_type=F32), 0.0).astype(BF16)

    def kv_finish(s, layer):
        qd_copy(s, 1, 1).wait()
        qx_copy(s, 1).wait()
        tot = (q_mine[s, 1, :, hw:3 * hw] + kd_recv[s, 1].astype(F32)) + kx_recv[s].astype(F32)
        k = (tot[:, 0:hw] + own_bias(bk_ref, layer)).astype(BF16)
        v = (tot[:, hw:2 * hw] + own_bias(bv_ref, layer)).astype(BF16)
        kfull[rsl(s), :hw] = k.astype(F32)
        vfull[rsl(s), :hw] = v.astype(F32)
        ke = jnp.dot(expand_mat(), k, preferred_element_type=F32)
        snew[...] = jnp.broadcast_to(jnp.sum(qblk[...].astype(F32) * ke, axis=1, keepdims=True), snew.shape)

    nr = CB * heads
    per = 128 // nr
    upper = lax.broadcasted_iota(jnp.int32, (8, 1), 0) < heads

    pos = lax.broadcasted_iota(jnp.int32, (nr, s_max), 1)

    def at_row(g):
        return pl.multiple_of(g * nr, nr)

    def scores_of(base, g):
        slot = lax.rem(base + g, RING)
        out = []
        for t in range(nr // 16):
            lhs = qblk[pl.ds(pl.multiple_of(at_row(g) + t * 16, 16), 16), :]
            d = [jnp.dot(lhs, kbuf[slot, t * 4 + i], preferred_element_type=F32)
                 for i in range(4)]
            out.append(jnp.where(upper, d[0][0:8], d[1][0:8]))
            out.append(jnp.where(upper, d[2][8:16], d[3][8:16]))
        return jnp.concatenate(out, axis=0)

    def softmax_of(s, g, sc):
        lens = []
        for i in range(0, CB, 2):
            b = s * rows + g * CB + i
            lens.append(jnp.where(upper, len_ref[b], len_ref[b + 1]))
        sc = jnp.where(pos < jnp.concatenate(lens, axis=0), sc, -jnp.inf)
        sn = snew[pl.ds(at_row(g), nr), 0:1]
        peak = jnp.maximum(jnp.max(sc, axis=1, keepdims=True), sn)
        e = jnp.exp(sc - peak)
        en = jnp.exp(sn - peak)
        inv = 1.0 / (jnp.sum(e, axis=1, keepdims=True) + en)
        return (e * inv).astype(BF16), jnp.broadcast_to(en * inv, (nr, LANES))

    def keep_probs(g, prob, fresh):
        for h in range(s_max // LANES):
            pbuf[h, pl.ds(at_row(g), nr), :] = prob[:, h * LANES:(h + 1) * LANES]
        pnew[pl.ds(at_row(g), nr), :] = fresh

    def probs_of(g):
        return wide([pbuf[h, pl.ds(pl.multiple_of(g // per * 128, 128), 128), :] for h in range(s_max // LANES)])

    def mix(base, g, rhs, new):
        slot = lax.rem(base + g, RING)
        seq = lax.broadcasted_iota(jnp.int32, (hw, 128), 1) // heads - lax.rem(g, per) * CB
        for b in range(CB):
            o = lax.dot_general(vbuf[slot, b], rhs, (((1,), (1,)), ((), ())), preferred_element_type=F32)
            new = jnp.where(seq == b, o, new)
        return new

    def refill(ci, i):
        @pl.when(ci + RING < total_chunks)
        def _():
            kv_start(ci + RING, i)

    def attention_pair(s, layer, g, tail):
        base = (layer * STREAMS + s) * nchunk
        kv_wait(base + g, 1)
        kv_wait(base + g + 1, 1)
        if not tail:
            kv_wait(base + g + 2, 0)
            kv_wait(base + g + 3, 0)
        sc = sbuf[...]
        rhs = probs_of(g)
        new = tmix[g // per]
        pa = softmax_of(s, g + 1, sc)
        if not tail:
            sc = scores_of(base, g + 2)
        new = mix(base, g, rhs, new)
        keep_probs(g + 1, *pa)
        rhs = probs_of(g + 1)
        if not tail:
            pa = softmax_of(s, g + 2, sc)
            sc = scores_of(base, g + 3)
        new = mix(base, g + 1, rhs, new)
        tmix[g // per] = new
        if not tail:
            keep_probs(g + 2, *pa)
            sbuf[...] = sc
        for k in range(2):
            refill(base + g + k, 1)
            if not tail:
                refill(base + g + 2 + k, 0)

    def open_ph(s, layer):
        base = (layer * STREAMS + s) * nchunk
        kv_wait(base, 0)
        kv_wait(base + 1, 0)
        first = scores_of(base, 0)
        second = scores_of(base, 1)
        kv_finish(s, layer)
        pa = softmax_of(s, 0, first)
        sbuf[...] = second
        keep_probs(0, *pa)
        refill(base, 0)
        refill(base + 1, 0)

    def attention(s, layer, lo, hi):

        def body(p, carry):
            attention_pair(s, layer, 2 * p, False)
            return carry

        stop = min(hi, nchunk - 2) // 2
        if stop - lo // 2 > 1:
            lax.fori_loop(lo // 2, stop, body, 0)
        elif stop > lo // 2:
            attention_pair(s, layer, lo, False)
        if hi == nchunk:
            attention_pair(s, layer, nchunk - 2, True)

    hrow = LANES // heads

    def att_copies(s, half):
        return [rcopy(att.at[s, r, half], att.at[s, r, half], at_ssem.at[s, i, half], at_rsem.at[s, i, half], dev)
                for i, dev in enumerate((dev_p, dev_x, dev_d))]

    def att_send(s, half):
        sel = (lax.broadcasted_iota(jnp.int32, (hrow, LANES), 1) // heads
               == lax.broadcasted_iota(jnp.int32, (hrow, LANES), 0)).astype(F32).astype(BF16)
        fresh = jnp.broadcast_to(pnew[half * LANES:(half + 1) * LANES, 0:1], (LANES, hw))
        pe = jnp.where(head_mask(LANES), fresh, 0.0).astype(BF16)
        first = s * rows + half * hrow
        o = jnp.dot(sel, pe, preferred_element_type=F32) * vfull[first:first + hrow, :hw]
        feat = lax.broadcasted_iota(jnp.int32, (hw, LANES), 0)
        lane = lax.rem(lax.broadcasted_iota(jnp.int32, (hw, LANES), 1), heads)
        t = jnp.where((feat >= lane * hd) & (feat < lane * hd + hd), tmix[half], 0.0)
        high = t.astype(BF16)
        low = (t - high.astype(F32)).astype(BF16)
        for part in (high, low):
            o = o + lax.dot_general(sel, part, (((1,), (1,)), ((), ())), preferred_element_type=F32)
        att[s, r, half] = o.astype(BF16)
        p, x, d = att_copies(s, half)
        x.start()
        d.start()
        p.start()

    def y_copy(s, which):
        return rcopy(ysend.at[which, s], yrecv.at[which, s], y_ssem.at[which, s], y_rsem.at[which, s], dev_y)

    def out_proj(s):
        for half in range(rows // hrow):
            for cp in att_copies(s, half):
                cp.wait()
        every = wide([jnp.concatenate([att[s, i, h] for h in range(rows // hrow)], axis=0) for i in range(4)])
        res = jnp.dot(every, wo[...], preferred_element_type=F32)
        ysend[0, s] = res.astype(BF16)
        y_copy(s, 0).start()

    def residual(s, which, bias):
        y_copy(s, which).wait()
        both = ysend[which, s].astype(F32) + yrecv[which, s].astype(F32)
        new = (state[rsl(s), :].astype(F32) + (both + bias.astype(F32))).astype(BF16)
        return new

    def fd_copy(s, j):
        return rcopy(fd_send.at[s, j], fd_recv.at[s, j], fd_ssem.at[s, j], fd_rsem.at[s, j], dev_p)

    def fx_copy(s, j):
        return rcopy(fx_send.at[s, j], fx_recv.at[s, j], fx_ssem.at[s, j], fx_rsem.at[s, j], dev_x)

    def u_copy(s, j, owner):
        return rcopy(u_buf.at[s, owner, j], u_buf.at[s, owner, j], u_ssem.at[s, j], u_rsem.at[s, j], dev_p)

    def fc1_part(s):
        yv = normed(s)

        def columns(owner, first, n):
            at = pl.multiple_of(owner * ff_half + first * LANES, LANES)
            return jnp.dot(yv, wf1[:, pl.ds(at, n * LANES)], preferred_element_type=F32)

        tiles = ff_half // LANES
        res = columns(1 - core, 0, tiles).astype(BF16)
        for j in range(nj):
            for t in range(ct):
                fd_send[s, j, t] = res[:, (j * ct + t) * LANES:(j * ct + t + 1) * LANES]
            fd_copy(s, j).start()
        res = columns(core, 0, tiles)
        for j in range(nj):
            f_mine[s, j] = res[:, j * CW:(j + 1) * CW]

    def fc1_forward(s, lo, hi):
        def body(j, carry):
            fd_copy(s, j).wait()
            for t in range(ct):
                fx_send[s, j, t] = (f_mine[s, j, :, t * LANES:(t + 1) * LANES] + fd_recv[s, j, t].astype(F32)).astype(BF16)
            fx_copy(s, j).start()
            return carry

        lax.fori_loop(lo, hi, body, 0)

    def fc2_dot(s, owner, lo, hi):
        off = pl.multiple_of(owner * ff_half + lo * CW, LANES)
        u = wide([u_buf[s, owner, j, t] for j in range(lo, hi) for t in range(ct)])
        return jnp.dot(u, wf2[pl.ds(off, (hi - lo) * CW), :], preferred_element_type=F32)

    def mlp(s, layer, lo, hi, plo, phi):
        def body(j, carry):
            fx_copy(s, j).wait()
            off = pl.multiple_of(core * ff_half + j * CW, LANES)
            bias = bf1_ref[layer:layer + 1, pl.ds(off, CW)].astype(F32)
            for t in range(ct):
                u = (fx_send[s, j, t].astype(F32) + fx_recv[s, j, t].astype(F32)) + bias[:, t * LANES:(t + 1) * LANES]
                u = u.astype(BF16)
                u_buf[s, core, j, t] = jnp.maximum(u, jnp.zeros_like(u))
            u_copy(s, j, core).start()
            return carry

        if hi == nj and hi - lo == 1:
            u_copy(s, plo, 1 - core).wait_recv()
            acc[s] += fc2_dot(s, 1 - core, plo, plo + 1)
            plo = plo + 1
        lax.fori_loop(lo, hi, body, 0)
        add = fc2_dot(s, core, lo, hi)
        if phi > plo:
            for j in range(plo, phi):
                u_copy(s, j, 1 - core).wait_recv()
            add = add + fc2_dot(s, 1 - core, plo, phi)
        if lo > 0:
            add = acc[s] + add
        if hi < nj:
            acc[s] = add
        else:
            ysend[1, s] = add.astype(BF16)
            y_copy(s, 1).start()
            for j in range(nj):
                u_copy(s, j, core).wait_send()

    def kv_out(layer):
        kt_ref[layer] = kfull[...].T[:hw, :].astype(BF16)
        vt_ref[layer] = vfull[...].T[:hw, :].astype(BF16)

    def gain_ph(s, which, layer):
        g, b = (g1_ref, c1_ref) if which == 0 else (g2_ref, c2_ref)
        norm(s, which, g[layer:layer + 1, :], b[layer:layer + 1, :])

    def mid_ph(s, layer):
        new = residual(s, 0, bo_ref[layer:layer + 1, :])
        state[rsl(s), :] = new
        stats_send(s, 1, new.astype(F32))

    def end_ph(s, layer):
        new = residual(s, 1, bf2_ref[layer:layer + 1, :])
        if layer == layers - 1:
            out_ref[rsl(s), :] = new
        else:
            state[rsl(s), :] = new
            stats_send(s, 0, new.astype(F32))

    one, two = range(STREAMS)
    small[0].wait()
    pl.semaphore_wait(barrier, 4)
    stats_send(one, 0, state[rsl(one), :].astype(F32))
    stats_send(two, 0, state[rsl(two), :].astype(F32))
    lax.fori_loop(0, RING, prime, 0)
    kfull[...] = jnp.zeros_like(kfull)
    vfull[...] = jnp.zeros_like(vfull)
    pbuf[...] = jnp.zeros_like(pbuf)
    tmix[...] = jnp.zeros_like(tmix)
    for cp in small[1:]:
        cp.wait()
    w_wait("qkv", 0)
    gain_ph(one, 0, 0)
    gain_ph(two, 0, 0)
    qkv_part(one, 0, 2)
    qkv_part(one, 1, 2)
    qkv_forward(one)
    qkv_forward(two)
    w_start("qkv", 1)
    w_start("o", 0)
    w_start("f1", 0)
    w_start("f2", 0)
    q_finish(one, 0)
    open_ph(one, 0)
    attention(one, 0, 0, nchunk // 2)
    att_send(one, 0)
    attention(one, 0, nchunk // 2, nchunk)
    att_send(one, 1)
    q4 = nchunk // 4
    for layer in range(layers):
        last = layer == layers - 1
        w_wait("o", layer)
        if last:
            out_proj(one)
        q_finish(two, layer)
        if last:
            open_ph(two, layer)
            attention(two, layer, 0, q4)
        else:
            open_ph(two, layer)
            attention(two, layer, 0, q4)
            out_proj(one)
        attention(two, layer, q4, 2 * q4)
        if last:
            mid_ph(one, layer)
        att_send(two, 0)
        attention(two, layer, 2 * q4, 3 * q4)
        if not last:
            mid_ph(one, layer)
        attention(two, layer, 3 * q4, nchunk)
        att_send(two, 1)
        w_wait("f1", layer)
        gain_ph(one, 1, layer)
        fc1_part(one)
        fc1_forward(one, 0, 3)
        out_proj(two)
        w_start("o", layer + 1)
        kv_out(layer)
        w_wait("f2", layer)
        mlp(one, layer, 0, 1, 0, 0)
        mid_ph(two, layer)
        fc1_forward(one, 3, nj)
        mlp(one, layer, 1, 2, 0, 1)
        mlp(one, layer, 2, 3, 1, 2)
        gain_ph(two, 1, layer)
        fc1_part(two)
        w_start("f1", layer + 1)
        fc1_forward(two, 0, nj if last else 4)
        mlp(one, layer, 3, nj, 2, nj)
        mlp(two, layer, 0, 1, 0, 0)
        end_ph(one, layer)
        if not last:
            fc1_forward(two, 4, nj)
        mlp(two, layer, 1, 2, 0, 1)
        if not last:
            w_wait("qkv", layer + 1)
            gain_ph(one, 0, layer + 1)
            qkv_part(one, 0)
            mlp(two, layer, 2, 3, 1, 2)
            qkv_forward(one)
            qkv_part(one, 1)
        else:
            mlp(two, layer, 2, 3, 1, 2)
        mlp(two, layer, 3, nj - 1, 2, 3)
        mlp(two, layer, nj - 1, nj, 3, nj)
        w_start("f2", layer + 1)
        if not last:
            q_finish(one, layer + 1)
            open_ph(one, layer + 1)
            attention(one, layer + 1, 0, q4)
            end_ph(two, layer)
            attention(one, layer + 1, q4, 2 * q4)
            att_send(one, 0)
            attention(one, layer + 1, 2 * q4, 3 * q4)
            gain_ph(two, 0, layer + 1)
            qkv_part(two, 0)
            attention(one, layer + 1, 3 * q4, nchunk)
            att_send(one, 1)
            qkv_forward(two)
            qkv_part(two, 1)
            w_start("qkv", layer + 2)
        else:
            end_ph(two, layer)


def finish(a_ref, b_ref, c_ref, x_ref, y_ref, z_ref, sem):
    copies = [pltpu.make_async_copy(a, b, sem.at[n])
              for n, (a, b) in enumerate(((a_ref, x_ref), (b_ref, y_ref), (c_ref, z_ref)))]
    for cp in copies:
        cp.start()
    for cp in copies:
        cp.wait()


def solution(mesh):
    act_spec = P("dp", "row")
    cache_spec = P(None, "dp", ("col", "row"), None, None)
    fresh_spec = P(None, "dp", ("col", "row"), None)
    in_weight = P(None, "row", "col")
    out_weight = P(None, "col", "row")
    col_vec = P(None, "col")
    row_vec = P(None, "row")
    in_specs = (act_spec, P("dp"), cache_spec, cache_spec, row_vec, row_vec,
                in_weight, col_vec, in_weight, col_vec, in_weight, col_vec,
                out_weight, row_vec, row_vec, row_vec, in_weight, col_vec, out_weight, row_vec)

    def local_step(hidden, cache_len, k_cache, v_cache, ln1_g, ln1_b, w_q, b_q, w_k, b_k, w_v, b_v,
                   w_o, b_o, ln2_g, ln2_b, w_fc1, b_fc1, w_fc2, b_fc2):
        layers, batch, heads, s_max, hd = k_cache.shape
        dm = hidden.shape[1]
        hw = heads * hd
        ff = w_fc1.shape[2]
        rows = batch // STREAMS
        nj = ff // 2 // CW
        nt = dm // LANES
        ct = CW // LANES
        kt = k_cache.transpose(0, 1, 2, 4, 3).reshape(layers, batch, hw, s_max)
        vt = v_cache.transpose(0, 1, 2, 4, 3).reshape(layers, batch, hw, s_max)
        vm = pl.BlockSpec(memory_space=pltpu.VMEM)
        hb = pl.BlockSpec(memory_space=pl.ANY)
        hr = heads * rows
        V = pltpu.VMEM
        D = pltpu.SemaphoreType.DMA
        scratch = [
            V((RING, CB, hw, s_max), BF16), V((RING, CB, hw, s_max), BF16),
            V((2, dm, 6 * hw), BF16), V(w_o.shape[1:], BF16), V(w_fc1.shape[1:], BF16), V(w_fc2.shape[1:], BF16),
            pltpu.SMEM((batch,), jnp.int32), V((layers, dm), BF16), V((layers, dm), BF16),
            V(b_q.shape, BF16), V(b_k.shape, BF16), V(b_v.shape, BF16), V(b_o.shape, BF16),
            V((layers, dm), BF16), V((layers, dm), BF16), V(b_fc1.shape, BF16), V(b_fc2.shape, BF16),
            V((batch, dm), BF16), V((nt, batch, LANES), BF16),
            V((2, STREAMS, 8, 2 * rows), F32), V((2, STREAMS, 3, 8, 2 * rows), F32),
            V((STREAMS, 2, rows, hw), BF16), V((STREAMS, 2, rows, hw), BF16), V((STREAMS, 2, rows, 2 * hw), BF16), V((STREAMS, 2, rows, 2 * hw), BF16),
            V((STREAMS, 2, rows, 3 * hw), F32),
            V((STREAMS, rows, hw), BF16), V((STREAMS, rows, hw), BF16), V((STREAMS, rows, 2 * hw), BF16), V((STREAMS, rows, 2 * hw), BF16),
            V((hr, hw), BF16), V((hr, 128), F32), V((CB * heads, s_max), F32), V((s_max // LANES, hr, LANES), BF16), V((hr, 128), F32),
            V((hr // 128, hw, 128), F32),
            V((STREAMS, 4, hr // LANES, LANES // heads, hw), BF16), V((batch, 384), F32), V((batch, 384), F32),
            V((2, STREAMS, rows, dm), BF16), V((2, STREAMS, rows, dm), BF16), V((STREAMS, rows, dm), F32),
            V((STREAMS, nj, ct, rows, LANES), BF16), V((STREAMS, nj, ct, rows, LANES), BF16), V((STREAMS, nj, rows, CW), F32),
            V((STREAMS, nj, ct, rows, LANES), BF16), V((STREAMS, nj, ct, rows, LANES), BF16),
            V((STREAMS, 2, nj, ct, rows, LANES), BF16),
            D((12,)), D((2, RING)), D((9,)), D((2, STREAMS, 3)), D((2, STREAMS, 3)),
            D((STREAMS, 2, 2)), D((STREAMS, 2, 2)), D((STREAMS, 2)), D((STREAMS, 2)),
            D((STREAMS, 3, hr // LANES)), D((STREAMS, 3, hr // LANES)), D((2, STREAMS)), D((2, STREAMS)),
            D((STREAMS, nj)), D((STREAMS, nj)), D((STREAMS, nj)), D((STREAMS, nj)), D((STREAMS, nj)), D((STREAMS, nj)),
        ]
        out, kn, vn = pl.pallas_call(
            functools.partial(fused, (layers, batch, dm, hw, heads, s_max, ff)),
            out_shape=(V((batch, dm), BF16), V((layers, hw, batch), BF16), V((layers, hw, batch), BF16)),
            in_specs=[hb] * 20,
            out_specs=(vm, vm, vm),
            scratch_shapes=scratch,
            compiler_params=pltpu.CompilerParams(collective_id=0, has_side_effects=True,
                                                 vmem_limit_bytes=60000000),
        )(hidden, cache_len, kt, vt, ln1_g, ln1_b, w_q, b_q, w_k, b_k, w_v, b_v,
          w_o, b_o, ln2_g, ln2_b, w_fc1, b_fc1, w_fc2, b_fc2)
        out, kn, vn = pl.pallas_call(
            finish, out_shape=tuple(jax.ShapeDtypeStruct(a.shape, a.dtype) for a in (out, kn, vn)),
            in_specs=[vm] * 3, out_specs=(hb,) * 3, scratch_shapes=[D((3,))],
            compiler_params=pltpu.CompilerParams(vmem_limit_bytes=4 << 20))(*(pltpu.with_memory_space_constraint(a, pltpu.VMEM) for a in (out, kn, vn)))
        kn = kn.reshape(layers, heads, hd, batch).transpose(0, 3, 1, 2)
        vn = vn.reshape(layers, heads, hd, batch).transpose(0, 3, 1, 2)
        return out, kn, vn

    return jax.shard_map(local_step, mesh=mesh, in_specs=in_specs,
                         out_specs=(act_spec, fresh_spec, fresh_spec), check_vma=False)
```
